32 devices in a mesh: group: 4 (over y, x), depth: 2 (over core), mp: 4 (over z).
Axes of the slice: x: 2, y: 2, z: 4, core: 2. Of those that a mesh axis runs over, the one named last changes fastest.
Arguments:
- states: bfloat16 [64, 4096], P(('group', 'depth', 'mp')), may hold values from -6 to 6
- queries: bfloat16 [64, 32, 128], P('group', 'mp'), may hold values from -6 to 6
- new_keys: bfloat16 [64, 8, 128], P('group', 'mp'), may hold values from -18 to 18
- new_values: bfloat16 [64, 8, 128], P('group', 'mp'), may hold values from -24 to 24
- text_keys: bfloat16 [64, 8, 512, 128], P('group', 'mp', 'depth'), may hold values from -6 to 6
- text_values: bfloat16 [64, 8, 512, 128], P('group', 'mp', 'depth'), may hold values from -24 to 24
- text_length: int32 [64], P('group'), may hold values from 2 to 512
- image_keys: bfloat16 [32, 8, 576, 128], P('group', 'mp'), may hold values from -6 to 6
- image_values: bfloat16 [32, 8, 576, 128], P('group', 'mp'), may hold values from -24 to 24
- image_slot: int32 [32], replicated, may hold values from 0 to 31, as said below
- block_list: int32 [4, 32], replicated, may hold values from 0 to 31, as said below
- block_count: int32 [4], replicated, may hold values from 16 to 32, as said below
- image_first: int32 [64], P('group'), may hold values from 0 to 31, as said below
- image_count: int32 [64], P('group'), may hold values from 1 to 2
- out_weight: bfloat16 [4096, 4096], P('mp'), may hold values from -0.09375 to 0.09375
- norm_gain: float32 [4096], replicated, may hold values from 0.5 to 1.5
- gate_weight: bfloat16 [4096, 14336], P(None, ('group', 'mp')), may hold values from -0.09375 to 0.09375
- up_weight: bfloat16 [4096, 14336], P(None, ('group', 'mp')), may hold values from -0.09375 to 0.09375
- down_weight: bfloat16 [14336, 4096], P(('group', 'mp')), may hold values from -0.046875 to 0.046875
Outputs:
- attention: bfloat16 [64, 32, 128], P(('group', 'depth'), 'mp')
- layer_out: bfloat16 [64, 4096], P(('group', 'depth', 'mp'))
The draws below stay inside these ranges and needn't reach their ends.
Inputs may be any that keep to these rules, and one draw needn't show every extreme that they name: `image_slot`: a permutation. The owner group of hash k is image_slot[k] // 8. `block_list`: the hashes of one group's list are distinct. Among one group's places with the same remainder modulo 2, at most 4 belongs to any one owner group; some group has block_count 32, and there every owner group holds exactly 4 place of every remainder. `block_count`: the sum of image_count over the group's requests. The requests of a group take consecutive list places in request order: image_first is the sum of image_count over the group's earlier requests.
All inputs are finite; a program needn't handle non-finite values.
Results may differ from the reference program's by a relative error of at most 0.012.
Values may be sent and summed in bfloat16 or wider, within the bound.
A program may use at most 128 MiB of HBM per device.

```python
import math
import jax
import jax.numpy as jnp
from jax import lax

D = 4096
HQ = 32
KVH = 8
HD = 128
FF = 14336
PATCHES = 576
REQ = 16
IMG_DEV = 8
GROUPS = 4
DEPTHS = 2
BATCH = 64
LTEXT = 512
IMAGES = 32
LIST = 32
CAP = 4


def routing_plan(key):
    slot_order = jax.random.permutation(jax.random.fold_in(key, 101), IMAGES).astype(jnp.int32)
    hash_at = jnp.argsort(slot_order, stable=True).astype(jnp.int32)
    picked = jax.random.randint(jax.random.fold_in(key, 102), (GROUPS, REQ), 1, 3, dtype=jnp.int32)
    fullest = jax.random.randint(jax.random.fold_in(key, 103), (), 0, GROUPS, dtype=jnp.int32)
    picked = jnp.where(jnp.arange(GROUPS, dtype=jnp.int32)[:, None] == fullest, 2, picked).astype(jnp.int32)
    starts = (jnp.cumsum(picked, axis=1) - picked).astype(jnp.int32)
    totals = jnp.sum(picked, axis=1).astype(jnp.int32)
    order_keys = jax.random.split(jax.random.fold_in(key, 104), GROUPS * DEPTHS)
    orderings = jax.vmap(lambda single: jax.random.permutation(single, GROUPS * CAP))(order_keys)
    orderings = orderings.reshape(GROUPS, DEPTHS, GROUPS * CAP).astype(jnp.int32)
    owners = orderings % GROUPS
    copy_index = orderings // GROUPS
    pick_keys = jax.random.split(jax.random.fold_in(key, 105), GROUPS * GROUPS)
    inner_orders = jax.vmap(lambda single: jax.random.permutation(single, IMG_DEV))(pick_keys)
    inner_orders = inner_orders.reshape(GROUPS, GROUPS, IMG_DEV).astype(jnp.int32)
    column = jnp.arange(DEPTHS, dtype=jnp.int32)[None, :, None] * CAP + copy_index
    group_axis = jnp.arange(GROUPS, dtype=jnp.int32)[:, None, None]
    within = inner_orders[group_axis, owners, column]
    slot_rows = owners * IMG_DEV + within
    hashes = hash_at[slot_rows]
    listing = jnp.transpose(hashes, (0, 2, 1)).reshape(GROUPS, LIST).astype(jnp.int32)
    return (slot_order, listing, totals, starts.reshape(-1), picked.reshape(-1))


def draw_image_slot(key, part):
    return routing_plan(key)[0]


def draw_block_list(key, part):
    return routing_plan(key)[1]


def draw_block_count(key, part):
    return routing_plan(key)[2]


def draw_image_first(key, part):
    return routing_plan(key)[3]


def draw_image_count(key, part):
    return routing_plan(key)[4]


def draw_queries(key, part):
    values = jnp.clip(jax.random.normal(jax.random.fold_in(key, 203), (BATCH, HQ, HD), jnp.float32), -6.0, 6.0)
    return values.astype(jnp.bfloat16)


def draw_text_keys(key, part):
    values = jnp.clip(jax.random.normal(jax.random.fold_in(key, 205), (BATCH, KVH, LTEXT, HD), jnp.float32), -6.0, 6.0)
    return values.astype(jnp.bfloat16)


def with_ends(drawn, rng, low, largest):
    longest = drawn.shape.index(max(drawn.shape))
    spots = []
    for shift in (0, 1):
        where = [jax.random.randint(jax.random.fold_in(rng, axis), (), 0, length) for axis, length in enumerate(drawn.shape)]
        where[longest] = (where[longest] + shift) % drawn.shape[longest]
        spots.append(tuple(where))
    return drawn.at[spots[0]].set(low).at[spots[1]].set(largest)


def steps_of(stream_key, shape, shards, least, high):
    level, own = 1.0, jax.random.fold_in(stream_key, 6)
    for position, parts in shards:
        draws = jnp.exp(jax.random.uniform(jax.random.fold_in(own, position), (parts,), jnp.float32, least / len(shards), high / len(shards)))
        level = level * jnp.repeat(draws, shape[position] // parts).reshape([-1 if axis == position else 1 for axis in range(len(shape))])
    return level


def gaussian(rng, extent, scale, limit, cuts=(), kind=jnp.bfloat16):
    factor_of = steps_of(rng, extent, cuts, -0.22, 0.18) if cuts else 1.0
    array = jax.random.normal(rng, extent, jnp.float32) * scale * factor_of
    return jnp.minimum(jnp.maximum(array, -limit), limit).astype(kind)


def setup_inputs(seed: int = 0) -> dict:
    keys = jax.random.split(jax.random.key(seed), 20)
    states = gaussian(keys[0], (BATCH, D), 1.0, 6.0, ((0, 32),))
    queries = draw_queries(jax.random.fold_in(keys[19], 71), 0)
    new_keys = gaussian(keys[2], (BATCH, KVH, HD), 3.0, 18.0, ((0, 4), (1, 4)))
    new_values = gaussian(keys[3], (BATCH, KVH, HD), 4.0, 24.0, ((0, 4), (1, 4)))
    text_keys = draw_text_keys(jax.random.fold_in(keys[19], 71), 0)
    text_values = gaussian(keys[5], (BATCH, KVH, LTEXT, HD), 4.0, 24.0, ((0, 4), (1, 4), (2, 2)))
    text_length = with_ends(jax.random.randint(keys[6], (BATCH,), 2, LTEXT + 1), jax.random.fold_in(keys[6], 1), 2, LTEXT).astype(jnp.int32)
    image_keys = gaussian(keys[7], (IMAGES, KVH, PATCHES, HD), 1.0, 6.0, ((0, 4), (1, 4)))
    image_values = gaussian(keys[8], (IMAGES, KVH, PATCHES, HD), 4.0, 24.0, ((0, 4), (1, 4)))
    image_slot = draw_image_slot(jax.random.fold_in(keys[19], 71), 0)
    block_list = draw_block_list(jax.random.fold_in(keys[19], 71), 0)
    block_count = draw_block_count(jax.random.fold_in(keys[19], 71), 0)
    image_first = draw_image_first(jax.random.fold_in(keys[19], 71), 0)
    image_count = draw_image_count(jax.random.fold_in(keys[19], 71), 0)
    out_weight = gaussian(keys[14], (HQ * HD, D), (HQ * HD) ** -0.5, 0.09375, ((0, 4),))
    norm_gain = jnp.clip(1.0 + 0.1 * jax.random.normal(keys[15], (D,), jnp.float32), 0.5, 1.5)
    gate_weight = gaussian(keys[16], (D, FF), D ** -0.5, 0.09375, ((1, 16),))
    up_weight = gaussian(keys[17], (D, FF), D ** -0.5, 0.09375, ((1, 16),))
    down_weight = gaussian(keys[18], (FF, D), FF ** -0.5, 0.046875, ((0, 16),))
    return dict(states=states, queries=queries, new_keys=new_keys, new_values=new_values, text_keys=text_keys, text_values=text_values, text_length=text_length, image_keys=image_keys, image_values=image_values, image_slot=image_slot, block_list=block_list, block_count=block_count, image_first=image_first, image_count=image_count, out_weight=out_weight, norm_gain=norm_gain, gate_weight=gate_weight, up_weight=up_weight, down_weight=down_weight)


LOG_TWO = math.log(2.0)
MASKED_SCORE = -1e+30
NORM_EPSILON = 1e-05

def reference(states, queries, new_keys, new_values, text_keys, text_values, text_length, image_keys, image_values, image_slot, block_list, block_count, image_first, image_count, out_weight, norm_gain, gate_weight, up_weight, down_weight):
    share = HQ // KVH
    scaling = 1.0 / math.sqrt(HD)

    def one_group(group_index):
        offset = (group_index * REQ).astype(jnp.int32)
        grouped = lax.dynamic_slice_in_dim(queries, offset, REQ, 0).astype(jnp.float32).reshape(REQ, KVH, share, HD)
        text_key_rows = lax.dynamic_slice_in_dim(text_keys, offset, REQ, 0).astype(jnp.float32)
        text_value_rows = lax.dynamic_slice_in_dim(text_values, offset, REQ, 0).astype(jnp.float32)
        new_key_rows = lax.dynamic_slice_in_dim(new_keys, offset, REQ, 0).astype(jnp.float32)
        new_value_rows = lax.dynamic_slice_in_dim(new_values, offset, REQ, 0).astype(jnp.float32)
        lengths = lax.dynamic_slice_in_dim(text_length, offset, REQ, 0)
        starts = lax.dynamic_slice_in_dim(image_first, offset, REQ, 0)
        image_total = lax.dynamic_slice_in_dim(image_count, offset, REQ, 0)
        hashes = block_list[group_index]
        slot_rows = jnp.take(image_slot, hashes, axis=0)
        image_key_rows = jnp.take(image_keys, slot_rows, axis=0).astype(jnp.float32)
        image_value_rows = jnp.take(image_values, slot_rows, axis=0).astype(jnp.float32)
        text_scores = jnp.einsum('rhgd,rhpd->rhgp', grouped, text_key_rows) * scaling
        new_scores = jnp.einsum('rhgd,rhd->rhg', grouped, new_key_rows) * scaling
        image_scores = jnp.einsum('rhgd,jhpd->rhgjp', grouped, image_key_rows) * scaling
        image_scores = image_scores.reshape(REQ, KVH, share, LIST * PATCHES)
        scores = jnp.concatenate([text_scores, new_scores[..., None], image_scores], axis=-1)
        text_mask = jnp.arange(LTEXT, dtype=jnp.int32)[None, :] < lengths[:, None]
        positions = jnp.arange(LIST, dtype=jnp.int32)[None, :]
        image_mask = (positions >= starts[:, None]) & (positions < (starts + image_total)[:, None]) & (positions < block_count[group_index])
        image_mask = jnp.repeat(image_mask, PATCHES, axis=1)
        new_mask = jnp.ones((REQ, 1), dtype=bool)
        allowed = jnp.concatenate([text_mask, new_mask, image_mask], axis=1)[:, None, None, :]
        masked = jnp.where(allowed, scores, MASKED_SCORE)
        highest = lax.optimization_barrier(jnp.max(masked, axis=-1, keepdims=True))
        levels = jnp.floor(highest / LOG_TWO)
        weights = jnp.where(allowed, jnp.exp(scores - LOG_TWO * levels), 0.0).astype(jnp.bfloat16)
        weights = lax.optimization_barrier(weights).astype(jnp.float32)
        totals = lax.optimization_barrier(jnp.sum(weights, axis=-1))
        text_weights = weights[..., :LTEXT]
        new_weights = weights[..., LTEXT]
        image_weights = weights[..., LTEXT + 1:].reshape(REQ, KVH, share, LIST, PATCHES)
        summed = jnp.einsum('rhgp,rhpd->rhgd', text_weights, text_value_rows)
        summed = summed + new_weights[..., None] * new_value_rows[:, :, None, :]
        summed = summed + jnp.einsum('rhgjp,jhpd->rhgd', image_weights, image_value_rows)
        return (summed / totals[..., None]).reshape(REQ, HQ, HD).astype(jnp.bfloat16)
    attention = lax.map(one_group, jnp.arange(GROUPS, dtype=jnp.int32)).reshape(BATCH, HQ, HD)
    projected = jnp.dot(attention.reshape(BATCH, HQ * HD), out_weight, preferred_element_type=jnp.float32)
    residual = states.astype(jnp.float32) + projected
    spread = lax.optimization_barrier(jnp.mean(residual * residual, axis=-1, keepdims=True))
    normed = (residual * lax.rsqrt(spread + NORM_EPSILON) * norm_gain.astype(jnp.float32)).astype(jnp.bfloat16)
    gate_term = jnp.dot(normed, gate_weight, preferred_element_type=jnp.float32)
    up_term = jnp.dot(normed, up_weight, preferred_element_type=jnp.float32)
    hidden = (jax.nn.silu(gate_term) * up_term).astype(jnp.bfloat16)
    result = residual + jnp.dot(hidden, down_weight, preferred_element_type=jnp.float32)
    return (attention, result.astype(jnp.bfloat16))
```

```python
import functools
import math

import jax
import jax.numpy as jnp
from jax import lax
from jax.experimental import pallas as pl
from jax.experimental.pallas import tpu as pltpu
from jax.sharding import PartitionSpec as P

LOG_TWO = math.log(2.0)
MASKED_SCORE = -1e30
NORM_EPSILON = 1e-05
READS = 2
DOWN_CHUNKS = 2
MESH = pl.DeviceIdType.MESH
F32 = jnp.float32
BF16 = jnp.bfloat16
I32 = jnp.int32
NT = (((1,), (1,)), ((), ()))


def kernel(
    dims,
    states_hbm,
    queries_hbm,
    new_keys_hbm,
    new_values_hbm,
    gain_hbm,
    text_length_hbm,
    image_slot_hbm,
    block_list_hbm,
    block_count_hbm,
    image_first_hbm,
    image_count_hbm,
    text_keys_hbm,
    text_values_hbm,
    image_keys_hbm,
    image_values_hbm,
    out_weight_hbm,
    gate_hbm,
    up_hbm,
    down_hbm,
    attention_out,
    layer_out,
    queries,
    new_keys,
    new_values,
    gain,
    text_length,
    image_slot,
    block_list,
    block_count,
    image_first,
    image_count,
    text_keys,
    text_values,
    image_keys,
    image_values,
    out_weight,
    gate,
    up,
    down,
    chosen,
    codes,
    states_recv,
    query_send,
    query_recv,
    text_scores,
    new_scores,
    text_weights,
    text_part,
    text_recv,
    image_send,
    stat_send,
    image_recv,
    stat_recv,
    merged,
    flat,
    proj_send,
    proj_recv,
    states_rows,
    res_cols,
    res_send,
    res_recv,
    x_all,
    square_all,
    gate_sum,
    up_sum,
    hidden,
    down_send,
    down_recv,
    load_sem,
    small_sem,
    state_ssem,
    state_rsem,
    query_ssem,
    query_rsem,
    text_ssem,
    text_rsem,
    image_ssem,
    image_rsem,
    stat_ssem,
    stat_rsem,
    proj_ssem,
    proj_rsem,
    x_ssem,
    x_rsem,
    square_ssem,
    square_rsem,
    res_ssem,
    res_rsem,
    down_ssem,
    down_rsem,
    ready_sem,
):
    groups, depths, mps = dims
    pieces = groups * mps
    g = lax.axis_index("group")
    d = lax.axis_index("depth")
    m = lax.axis_index("mp")
    requests, heads, width = queries.shape
    kv_heads, span = text_keys.shape[1], text_keys.shape[2]
    share = heads // kv_heads
    stored, patches = image_keys.shape[0], image_keys.shape[2]
    listed = block_list.shape[1]
    steps = listed // depths
    copies = listed // (depths * groups)
    places = groups * copies
    per_depth = requests // depths
    rows = states_recv.shape[1]
    model = layer_out.shape[1]
    cols = model // mps
    chunks, part_cols = down_recv.shape[1], down_recv.shape[3]
    scaling = 1.0 / math.sqrt(width)
    far = [(m + k) % mps for k in range(1, mps)]
    if mps % 2 == 0:
        half = m // (mps // 2)
        far = [
            (1 - half) * (mps - 1 - k - (m + k) // (mps - 1)) + half * (k + (mps - 1 + k - m) // (mps - 1))
            for k in range(mps - 1)
        ]
    near = list(reversed(far))
    plane = [(g + k) % groups for k in range(1, groups)]

    barrier = pltpu.get_barrier_semaphore()

    def tell(sem, gg, dd, mm):
        pl.semaphore_signal(sem, inc=1, device_id=(gg, dd, mm), device_id_type=MESH)

    for peer in far:
        tell(barrier, g, d, peer)
    for peer in plane:
        tell(barrier, peer, d, m)
    for e in range(1, depths):
        for k in range(groups):
            tell(barrier, (g + k) % groups, (d + e) % depths, m)

    own_columns = pl.ds(pl.multiple_of(m * cols, cols), cols)
    small_pairs = (
        (image_slot_hbm, image_slot),
        (block_list_hbm, block_list),
        (block_count_hbm, block_count),
        (image_first_hbm, image_first),
        (image_count_hbm, image_count),
        (text_length_hbm, text_length),
        (queries_hbm, queries),
        (new_keys_hbm, new_keys),
        (new_values_hbm, new_values),
        (gain_hbm.at[:, own_columns], gain),
        (states_hbm.at[:, own_columns], states_recv.at[m]),
    )
    smalls = [pltpu.make_async_copy(a, b, small_sem.at[i]) for i, (a, b) in enumerate(small_pairs)]
    for small in smalls:
        small.start()
    pairs = (
        (text_keys_hbm, text_keys),
        (text_values_hbm, text_values),
        (image_keys_hbm, image_keys),
        (image_values_hbm, image_values),
        (out_weight_hbm, out_weight),
        (gate_hbm, gate),
        (up_hbm, up),
        (down_hbm, down),
    )
    loads = [pltpu.make_async_copy(a, b, load_sem.at[i]) for i, (a, b) in enumerate(pairs)]
    for load in loads[:4]:
        load.start()

    def remote(src, dst, ssem, rsem, gg, dd, mm):
        return pltpu.make_async_remote_copy(
            src_ref=src,
            dst_ref=dst,
            send_sem=ssem,
            recv_sem=rsem,
            device_id=(gg, dd, mm),
            device_id_type=MESH,
        )

    for small in smalls[:6]:
        small.wait()

    own_count = block_count[g]
    counts = [jnp.int32(0)] * (depths * groups)
    for place in range(listed):
        p = place % depths
        owner = lax.div(image_slot[block_list[g, place]], jnp.int32(stored))
        live = (place < own_count).astype(I32)
        rank = jnp.int32(0)
        for o in range(groups):
            mine = owner == o
            rank = jnp.where(mine, counts[p * groups + o], rank)
            counts[p * groups + o] = counts[p * groups + o] + jnp.where(mine, live, 0)
        codes[place] = jnp.minimum(owner * copies + rank, places - 1)

    def wanted(r):
        found = jnp.int32(-1)
        for k in range(READS):
            place = image_first[r] + k
            held = jnp.minimum(place, listed - 1)
            good = (k < image_count[r]) & (place < own_count) & (lax.rem(place, depths) == d)
            found = jnp.where(good, codes[held], found)
        return found

    smalls[6].wait()
    picked = [jnp.zeros((heads, width), F32)] * places
    for r in range(requests):
        code = jnp.full((heads, width), wanted(r), I32)
        q = queries[r].astype(F32)
        picked = [jnp.where(code == i, q, old) for i, old in enumerate(picked)]
    for o in range(groups):
        for c in range(copies):
            query_send[o, c] = picked[o * copies + c].astype(BF16)
    query_recv[g] = query_send[g]

    pl.semaphore_wait(barrier, groups - 1 + (depths - 1) * groups + mps - 1)

    def query_copy(peer, slot):
        return remote(
            query_send.at[peer], query_recv.at[slot], query_ssem, query_rsem.at[slot], peer, d, m
        )

    for peer in plane:
        query_copy(peer, g).start()
    for peer in far:
        tell(ready_sem, g, d, peer)

    def state_copy(peer):
        columns = pl.ds(pl.multiple_of(peer * cols, cols), cols)
        return remote(
            states_hbm.at[:, columns], states_recv.at[m], state_ssem, state_rsem, g, d, peer
        )

    for peer in far:
        state_copy(peer).start()

    def serve_step(i, state):
        place = i * depths + d
        out = []
        for s in range(groups):
            rank, held = state[s]
            slot = image_slot[block_list[s, place]]
            hit = (lax.div(slot, jnp.int32(stored)) == g) & (place < block_count[s])
            within = lax.rem(slot, jnp.int32(stored))
            target = jnp.where(hit, rank, -1)
            held = tuple(jnp.where(target == c, within, old) for c, old in enumerate(held))
            out.append((rank + hit.astype(I32), held))
        return tuple(out)

    zero = jnp.int32(0)
    served = lax.fori_loop(0, steps, serve_step, ((zero, (zero,) * copies),) * groups, unroll=2)
    for s in range(groups):
        for c in range(copies):
            chosen[s * copies + c] = served[s][1][c]

    def by_head(parts):
        result = parts[0]
        row = lax.broadcasted_iota(I32, result.shape, 0)
        for h in range(1, kv_heads):
            result = jnp.where(row >= h * share, parts[h], result)
        return result

    def spread_rows(small):
        return by_head(
            [jnp.broadcast_to(small[h : h + 1, :], (heads, width)) for h in range(kv_heads)]
        )

    def widen(q):
        full = q.astype(F32)
        row = lax.broadcasted_iota(I32, full.shape, 0)
        parts = [
            jnp.where((row >= h * share) & (row < (h + 1) * share), full, 0.0)
            for h in range(kv_heads)
        ]
        return jnp.concatenate(parts, axis=1).astype(BF16)

    def joined(ref, index):
        return jnp.concatenate([ref[index, h] for h in range(kv_heads)], axis=1)

    def split_heads(wide):
        return by_head([wide[:, h * width : (h + 1) * width] for h in range(kv_heads)])

    smalls[7].wait()
    smalls[8].wait()
    loads[0].wait()
    loads[4].start()
    lanes = lax.broadcasted_iota(I32, (heads, span), 1) + d * span

    def text_first(r, carry):
        q = queries[r]
        score = lax.dot_general(widen(q), joined(text_keys, r), NT, preferred_element_type=F32)
        text_scores[r] = jnp.where(lanes < text_length[r], score * scaling, MASKED_SCORE)
        key = spread_rows(new_keys[r].astype(F32))
        new_score = jnp.sum(q.astype(F32) * key, axis=-1, keepdims=True) * scaling
        new_scores[r] = jnp.broadcast_to(new_score, (heads, width))
        return carry

    lax.fori_loop(0, requests, text_first, 0, unroll=4)
    is_first = jnp.full((requests, heads, width), d, I32) == 0
    score = text_scores[...]
    fresh = jnp.where(is_first, new_scores[...], MASKED_SCORE)
    top = jnp.maximum(jnp.max(score, axis=-1, keepdims=True), fresh)
    level = jnp.floor(top / LOG_TWO)
    text_part[:, 1] = level
    weight = jnp.where(
        score > 0.5 * MASKED_SCORE, jnp.exp(score - LOG_TWO * level[:, :, :1]), 0.0
    ).astype(BF16)
    text_weights[...] = weight
    fresh_weight = jnp.where(is_first, jnp.exp(new_scores[...] - LOG_TWO * level), 0.0)
    fresh_weight = fresh_weight.astype(BF16).astype(F32)
    new_scores[...] = fresh_weight
    text_part[:, 2] = jnp.sum(weight.astype(F32), axis=-1, keepdims=True) + fresh_weight
    loads[1].wait()

    def text_second(r, carry):
        wide = jnp.dot(text_weights[r], joined(text_values, r), preferred_element_type=F32)
        fresh_value = new_scores[r] * spread_rows(new_values[r].astype(F32))
        text_part[r, 0] = split_heads(wide) + fresh_value
        return carry

    lax.fori_loop(0, requests, text_second, 0, unroll=4)

    def text_copy(peer, slot):
        return remote(
            text_part.at[pl.ds(peer * per_depth, per_depth)],
            text_recv.at[slot],
            text_ssem,
            text_rsem.at[slot],
            g,
            peer,
            m,
        )

    others = [(d + e) % depths for e in range(1, depths)]
    for other in others:
        text_copy(other, d).start()
    for load in loads[5:]:
        load.start()
    text_recv[d] = text_part[pl.ds(d * per_depth, per_depth)]

    loads[2].wait()
    loads[3].wait()
    stat_lane = lax.broadcasted_iota(I32, (heads, width), 1)
    stat_row = lax.broadcasted_iota(I32, (heads, width), 0)
    own_lane = lax.rem(stat_lane, heads) == stat_row
    stat_kind = lax.div(stat_lane, heads)

    def serve(s):
        slots = [chosen[s * copies + c] for c in range(copies)]
        scores = [
            scaling
            * lax.dot_general(
                widen(query_recv[s, c]),
                joined(image_keys, slots[c]),
                NT,
                preferred_element_type=F32,
            )
            for c in range(copies)
        ]
        stats = jnp.zeros((heads, width), F32)
        weights = []
        for c in range(copies):
            level = jnp.floor(jnp.max(scores[c], axis=-1, keepdims=True) / LOG_TWO)
            weight = jnp.exp(scores[c] - LOG_TWO * level).astype(BF16)
            total = jnp.sum(weight.astype(F32), axis=-1, keepdims=True)
            stats = jnp.where(stat_kind == 2 * c, level, stats)
            stats = jnp.where(stat_kind == 2 * c + 1, total, stats)
            weights.append(weight)
        stat_send[s] = jnp.sum(jnp.where(own_lane, stats, 0.0), axis=0, keepdims=True)
        for c in range(copies):
            wide = jnp.dot(weights[c], joined(image_values, slots[c]), preferred_element_type=F32)
            image_send[s, c] = split_heads(wide).astype(BF16)

    def image_copy(peer, depth):
        return remote(
            image_send.at[peer],
            image_recv.at[pl.ds((d * groups + g) * copies, copies)],
            image_ssem,
            image_rsem,
            peer,
            depth,
            m,
        )

    def stat_copy(peer, depth):
        return remote(
            stat_send.at[peer],
            stat_recv.at[d * groups + g],
            stat_ssem,
            stat_rsem,
            peer,
            depth,
            m,
        )

    serve(g)
    stat_recv[d * groups + g] = stat_send[g]
    image_recv[pl.ds((d * groups + g) * copies, copies)] = image_send[g]
    for other in others:
        image_copy(g, other).start()
        stat_copy(g, other).start()

    def serve_other(k, carry):
        s = lax.rem(g + k, groups)
        query_copy(s, s).wait_recv()
        serve(s)
        for e in range(depths):
            image_copy(s, lax.rem(d + e, depths)).start()
            stat_copy(s, lax.rem(d + e, depths)).start()
        return carry

    lax.fori_loop(1, groups, serve_other, 0, unroll=True)

    remote(states_recv.at[pl.ds(0, mps - 1)], states_recv.at[pl.ds(0, mps - 1)], state_ssem, state_rsem, g, d, m).wait_recv()
    smalls[9].wait()
    smalls[10].wait()
    for i in range(mps):
        states_rows[i * rows : (i + 1) * rows, :] = states_recv[i].astype(F32)

    for other in others:
        text_copy(other, other).wait_recv()
    arrivals = depths * groups - 1
    image_all = image_recv.at[pl.ds(0, arrivals * copies)]
    stat_all = stat_recv.at[pl.ds(0, arrivals)]
    remote(stat_all, stat_all, stat_ssem, stat_rsem, g, d, m).wait_recv()
    remote(image_all, image_all, image_ssem, image_rsem, g, d, m).wait_recv()

    def stat_of(stats, lane):
        picked = jnp.sum(jnp.where(stat_lane == lane + stat_row, stats, 0.0), axis=-1, keepdims=True)
        return jnp.broadcast_to(picked, (heads, width))

    def merge(i, carry):
        r = d * per_depth + i
        parts = [tuple(text_recv[e, i, n] for n in range(3)) for e in range(depths)]
        for k in range(READS):
            place = image_first[r] + k
            good = (k < image_count[r]) & (place < own_count)
            held = jnp.minimum(place, listed - 1)
            code = codes[held]
            at = lax.rem(held, depths)
            owner = lax.div(code, jnp.int32(copies))
            rank = lax.rem(code, jnp.int32(copies))
            stats = jnp.broadcast_to(stat_recv[at * groups + owner], (heads, width))
            live = jnp.full((heads, width), good.astype(I32), I32) == 1
            parts.append(
                (
                    jnp.where(live, image_recv[at * places + code].astype(F32), 0.0),
                    jnp.where(live, stat_of(stats, 2 * rank * heads), MASKED_SCORE),
                    jnp.where(live, stat_of(stats, (2 * rank + 1) * heads), 0.0),
                )
            )
        highest = functools.reduce(jnp.maximum, [part[1] for part in parts])
        factors = [jnp.exp2(part[1] - highest) for part in parts]
        total = sum(part[2] * factor for part, factor in zip(parts, factors))
        value = sum(part[0] * factor for part, factor in zip(parts, factors)) / total
        merged[i] = value
        attention_out[i] = value.astype(BF16)
        return carry

    lax.fori_loop(0, per_depth, merge, 0, unroll=True)
    for h in range(heads):
        flat[:, h * width : (h + 1) * width] = merged[:, h, :]

    loads[4].wait()
    low = flat[...].astype(BF16)

    def project(block):
        columns = pl.ds(pl.multiple_of(block * cols, cols), cols)
        return jnp.dot(low, out_weight[:, columns], preferred_element_type=F32)

    def proj_copy(k, peer):
        return remote(proj_send.at[k], proj_recv.at[m], proj_ssem, proj_rsem, g, d, peer)

    for k, peer in enumerate(far):
        proj_send[k] = project(peer).astype(BF16)
        proj_copy(k, peer).start()
    total = project(m) + states_rows[...]
    sent = proj_send.at[pl.ds(0, mps - 1)]
    remote(sent, proj_recv.at[pl.ds(0, mps - 1)], proj_ssem, proj_rsem, g, d, m).wait_recv()
    for k in range(1, mps):
        total = total + proj_recv[lax.rem(m + k, mps)].astype(F32)
    res_cols[...] = total
    me = m * groups + g
    x_all[me] = (total * gain[...]).astype(BF16)
    square = jnp.broadcast_to(jnp.sum(total * total, axis=-1, keepdims=True), (per_depth, width))
    square_lane = lax.broadcasted_iota(I32, (per_depth, width), 1)
    square_row = lax.broadcasted_iota(I32, (per_depth, width), 0)
    diagonal = square_lane == square_row
    square_all[me] = jnp.sum(jnp.where(diagonal, square, 0.0), axis=0, keepdims=True)

    pl.semaphore_wait(ready_sem, mps - 1)

    def x_copy(gg, mm):
        return remote(x_all.at[me], x_all.at[me], x_ssem, x_rsem.at[m], gg, d, mm)

    def square_copy(gg, mm):
        return remote(square_all.at[me], square_all.at[me], square_ssem, square_rsem, gg, d, mm)

    targets = [(peer, m) for peer in plane]
    for block in far:
        targets += [((g + k) % groups, block) for k in range(groups)]
    for gg, mm in targets:
        x_copy(gg, mm).start()
    for gg, mm in targets:
        square_copy(gg, mm).start()

    for i in range(mps):
        res_send[i] = res_cols[i * rows : (i + 1) * rows, :]

    def res_copy(peer):
        return remote(res_send.at[peer], res_recv.at[m], res_ssem, res_rsem, g, d, peer)

    for peer in far:
        res_copy(peer).start()
    res_recv[m] = res_send[m]

    loads[5].wait()
    loads[6].wait()
    loads[7].wait()

    def expand(block, first):
        tokens = [x_all[block * groups + s].astype(F32) for s in range(groups)]
        tokens = jnp.concatenate(tokens, axis=0).astype(BF16)
        part = pl.ds(pl.multiple_of(block * cols, cols), cols)
        a = jnp.dot(tokens, gate[part, :], preferred_element_type=F32)
        b = jnp.dot(tokens, up[part, :], preferred_element_type=F32)
        if first:
            gate_sum[...] = a
            up_sum[...] = b
        else:
            gate_sum[...] += a
            up_sum[...] += b

    def x_wait(block, count):
        got = x_all.at[pl.ds(0, count)]
        remote(got, got, x_ssem, x_rsem.at[block], g, d, m).wait_recv()

    x_wait(m, groups - 1)
    expand(m, True)
    for i, block in enumerate([lax.rem(m + k, mps) for k in range(1, mps)]):
        if i == mps - 2:
            got = square_all.at[pl.ds(0, pieces - 1)]
            remote(got, got, square_ssem, square_rsem, g, d, m).wait_recv()
            scales = []
            for s in range(groups):
                row = sum(square_all[i2 * groups + s] for i2 in range(mps))
                row = jnp.broadcast_to(row, (per_depth, width))
                mean = jnp.sum(jnp.where(diagonal, row, 0.0), axis=-1, keepdims=True) / model
                scales.append(lax.rsqrt(mean + NORM_EPSILON))
            scale = jnp.concatenate(scales, axis=0)
        x_wait(block, groups)
        expand(block, False)
    v = gate_sum[...] * scale
    hidden[...] = (v / (1.0 + jnp.exp(-v)) * (up_sum[...] * scale)).astype(BF16)

    def down_copy(n, gg, mm):
        return remote(
            down_send.at[n, mm * groups + gg],
            down_recv.at[me, n],
            down_ssem,
            down_rsem,
            gg,
            d,
            mm,
        )

    order = targets[groups - 1 :] + targets[: groups - 1]
    for n in range(chunks):
        columns = slice(n * part_cols, (n + 1) * part_cols)
        part = jnp.dot(hidden[...], down[:, columns], preferred_element_type=F32)
        for s in range(groups):
            for i in range(mps):
                at = s * per_depth + i * rows
                down_send[n, i * groups + s] = part[at : at + rows, :].astype(BF16)
        for gg, mm in order:
            down_copy(n, gg, mm).start()
    down_recv[me] = down_send[:, me]

    got = res_recv.at[pl.ds(0, mps - 1)]
    remote(got, got, res_ssem, res_rsem, g, d, m).wait_recv()
    got = down_recv.at[pl.ds(0, pieces - 1)]
    remote(got, got, down_ssem, down_rsem, g, d, m).wait_recv()

    for n in range(chunks):

        def add_piece(i, total):
            return total + down_recv[i, n].astype(F32)

        summed = lax.fori_loop(0, pieces, add_piece, jnp.zeros((rows, part_cols), F32), unroll=4)
        for i in range(mps):
            low_edge, high_edge = max(n * part_cols, i * cols), min((n + 1) * part_cols, (i + 1) * cols)
            if low_edge < high_edge:
                layer_out[:, low_edge:high_edge] = (
                    summed[:, low_edge - n * part_cols : high_edge - n * part_cols]
                    + res_recv[i, :, low_edge - i * cols : high_edge - i * cols]
                ).astype(BF16)

    def sent_all(ref, ssem, rsem):
        remote(ref, ref, ssem, rsem, g, d, m).wait_send()

    sent_all(states_recv.at[pl.ds(0, mps - 1)], state_ssem, state_rsem)
    sent_all(query_send.at[pl.ds(0, groups - 1)], query_ssem, query_rsem.at[0])
    for other in others:
        text_copy(other, d).wait_send()
    sent_all(image_all, image_ssem, image_rsem)
    sent_all(stat_all, stat_ssem, stat_rsem)
    sent_all(proj_send.at[pl.ds(0, mps - 1)], proj_ssem, proj_rsem)
    sent_all(x_all.at[pl.ds(0, pieces - 1)], x_ssem, x_rsem.at[0])
    sent_all(square_all.at[pl.ds(0, pieces - 1)], square_ssem, square_rsem)
    sent_all(res_send.at[pl.ds(0, mps - 1)], res_ssem, res_rsem)
    sent_all(down_recv.at[pl.ds(0, pieces - 1)], down_ssem, down_rsem)


def finish(attention, layer, attention_out, layer_out):
    attention_out[...] = attention[...]
    layer_out[...] = layer[...]


def on_device(
    states,
    queries,
    new_keys,
    new_values,
    text_keys,
    text_values,
    text_length,
    image_keys,
    image_values,
    image_slot,
    block_list,
    block_count,
    image_first,
    image_count,
    out_weight,
    norm_gain,
    gate_weight,
    up_weight,
    down_weight,
):
    groups = lax.axis_size("group")
    depths = lax.axis_size("depth")
    mps = lax.axis_size("mp")
    pieces = groups * mps
    requests, heads, width = queries.shape
    listed = block_list.shape[1]
    copies = listed // (depths * groups)
    per_depth = requests // depths
    rows, model = states.shape
    cols = model // mps
    units = gate_weight.shape[1]
    span = text_keys.shape[2]
    part_cols = model // DOWN_CHUNKS
    dma = pltpu.SemaphoreType.DMA
    vmem = pl.BlockSpec(memory_space=pltpu.VMEM)
    hbm = pl.BlockSpec(memory_space=pl.ANY)
    small = (
        states,
        queries,
        new_keys,
        new_values,
        norm_gain.reshape(1, model),
        text_length,
        image_slot,
        block_list,
        block_count,
        image_first,
        image_count,
    )
    big = (
        text_keys,
        text_values,
        image_keys,
        image_values,
        out_weight,
        gate_weight,
        up_weight,
        down_weight,
    )
    scratch = [pltpu.VMEM(a.shape, a.dtype) for a in small[1:4]]
    scratch += [pltpu.VMEM((1, cols), norm_gain.dtype)]
    scratch += [pltpu.SMEM(a.shape, a.dtype) for a in small[5:]]
    scratch += [pltpu.VMEM(a.shape, a.dtype) for a in big]
    scratch += [
        pltpu.SMEM((groups * copies,), I32),
        pltpu.SMEM((listed,), I32),
        pltpu.VMEM((mps, rows, cols), BF16),
        pltpu.VMEM((groups, copies, heads, width), BF16),
        pltpu.VMEM((groups, copies, heads, width), BF16),
        pltpu.VMEM((requests, heads, span), F32),
        pltpu.VMEM((requests, heads, width), F32),
        pltpu.VMEM((requests, heads, span), BF16),
        pltpu.VMEM((requests, 3, heads, width), F32),
        pltpu.VMEM((depths, per_depth, 3, heads, width), F32),
        pltpu.VMEM((groups, copies, heads, width), BF16),
        pltpu.VMEM((groups, 1, width), F32),
        pltpu.VMEM((depths * groups * copies, heads, width), BF16),
        pltpu.VMEM((depths * groups, 1, width), F32),
        pltpu.VMEM((per_depth, heads, width), F32),
        pltpu.VMEM((per_depth, heads * width), F32),
        pltpu.VMEM((mps, per_depth, cols), BF16),
        pltpu.VMEM((mps, per_depth, cols), BF16),
        pltpu.VMEM((per_depth, cols), F32),
        pltpu.VMEM((per_depth, cols), F32),
        pltpu.VMEM((mps, rows, cols), F32),
        pltpu.VMEM((mps, rows, cols), F32),
        pltpu.VMEM((pieces, per_depth, cols), BF16),
        pltpu.VMEM((pieces, 1, width), F32),
        pltpu.VMEM((groups * per_depth, units), F32),
        pltpu.VMEM((groups * per_depth, units), F32),
        pltpu.VMEM((groups * per_depth, units), BF16),
        pltpu.VMEM((DOWN_CHUNKS, pieces, rows, part_cols), BF16),
        pltpu.VMEM((pieces, DOWN_CHUNKS, rows, part_cols), BF16),
        dma((len(big),)),
        dma((len(small),)),
        dma,
        dma,
        dma,
        dma((groups,)),
        dma,
        dma((depths,)),
        dma,
        dma,
        dma,
        dma,
        dma,
        dma,
        dma,
        dma((mps,)),
        dma,
        dma,
        dma,
        dma,
        dma,
        dma,
        pltpu.SemaphoreType.REGULAR,
    ]
    raw = pl.pallas_call(
        functools.partial(kernel, (groups, depths, mps)),
        out_shape=(
            pltpu.VMEM((per_depth, heads, width), BF16),
            pltpu.VMEM((rows, model), BF16),
        ),
        in_specs=[hbm] * 19,
        out_specs=(vmem, vmem),
        scratch_shapes=scratch,
        compiler_params=pltpu.CompilerParams(
            collective_id=0, has_side_effects=True, vmem_limit_bytes=60000000
        ),
    )(*small, *big)
    return pl.pallas_call(
        finish,
        out_shape=(
            jax.ShapeDtypeStruct((per_depth, heads, width), BF16),
            jax.ShapeDtypeStruct((rows, model), BF16),
        ),
        in_specs=[vmem] * 2,
        out_specs=(vmem, vmem),
    )(*(pltpu.with_memory_space_constraint(r, pltpu.VMEM) for r in raw))


def solution(mesh):
    placed = (
        P(("group", "depth", "mp"), None),
        P("group", "mp", None),
        P("group", "mp", None),
        P("group", "mp", None),
        P("group", "mp", "depth", None),
        P("group", "mp", "depth", None),
        P("group"),
        P("group", "mp", None, None),
        P("group", "mp", None, None),
        P(),
        P(),
        P(),
        P("group"),
        P("group"),
        P("mp", None),
        P(),
        P(None, ("group", "mp")),
        P(None, ("group", "mp")),
        P(("group", "mp"), None),
    )
    return jax.shard_map(
        on_device,
        mesh=mesh,
        in_specs=placed,
        out_specs=(P(("group", "depth"), "mp", None), P(("group", "depth", "mp"), None)),
        check_vma=False,
    )
```

```python
import functools
import math

import jax
import jax.numpy as jnp
from jax import lax
from jax.experimental import pallas as pl
from jax.experimental.pallas import tpu as pltpu
from jax.sharding import PartitionSpec as P

LOG_TWO = math.log(2.0)
MASKED_SCORE = -1e30
NORM_EPSILON = 1e-05
READS = 2
DOWN_CHUNKS = 1
MESH = pl.DeviceIdType.MESH
F32 = jnp.float32
BF16 = jnp.bfloat16
I32 = jnp.int32
NT = (((1,), (1,)), ((), ()))


def kernel(
    dims,
    states_hbm,
    queries_hbm,
    new_keys_hbm,
    new_values_hbm,
    gain_hbm,
    text_length_hbm,
    image_slot_hbm,
    block_list_hbm,
    block_count_hbm,
    image_first_hbm,
    image_count_hbm,
    text_keys_hbm,
    text_values_hbm,
    image_keys_hbm,
    image_values_hbm,
    out_weight_hbm,
    gate_hbm,
    up_hbm,
    down_hbm,
    attention_out,
    layer_out,
    queries,
    new_keys,
    new_values,
    gain,
    text_length,
    image_slot,
    block_list,
    block_count,
    image_first,
    image_count,
    text_keys,
    text_values,
    image_keys,
    image_values,
    out_weight,
    gate,
    up,
    down,
    chosen,
    codes,
    states_recv,
    query_send,
    query_recv,
    text_scores,
    new_scores,
    text_weights,
    text_part,
    text_recv,
    image_send,
    stat_send,
    image_recv,
    stat_recv,
    merged,
    flat,
    proj_send,
    proj_recv,
    states_rows,
    res_cols,
    res_send,
    res_recv,
    x_all,
    square_cols,
    square_all,
    gate_sum,
    up_sum,
    hidden,
    down_send,
    down_recv,
    load_sem,
    small_sem,
    state_ssem,
    state_rsem,
    query_ssem,
    query_rsem,
    text_ssem,
    text_rsem,
    image_ssem,
    image_rsem,
    stat_ssem,
    stat_rsem,
    proj_ssem,
    proj_rsem,
    x_ssem,
    x_rsem,
    hand_rsem,
    square_ssem,
    square_rsem,
    res_ssem,
    res_rsem,
    down_ssem,
    down_rsem,
    ready_sem,
):
    groups, depths, mps = dims
    pieces = groups * mps
    g = lax.axis_index("group")
    d = lax.axis_index("depth")
    m = lax.axis_index("mp")
    requests, heads, width = queries.shape
    kv_heads, span = text_keys.shape[1], text_keys.shape[2]
    share = heads // kv_heads
    stored, patches = image_keys.shape[0], image_keys.shape[2]
    listed = block_list.shape[1]
    steps = listed // depths
    copies = listed // (depths * groups)
    places = groups * copies
    per_depth = requests // depths
    rows = states_recv.shape[1]
    model = layer_out.shape[1]
    cols = model // mps
    chunks, part_cols = down_recv.shape[1], down_recv.shape[3]
    scaling = 1.0 / math.sqrt(width)
    far = [lax.rem(m + k, mps) for k in range(1, mps)]
    if mps % 2 == 0:
        half = lax.div(m, mps // 2)
        far = [
            (1 - half) * (mps - 1 - k - lax.div(m + k, mps - 1))
            + half * (k + lax.div(mps - 1 + k - m, mps - 1))
            for k in range(mps - 1)
        ]
    near = [lax.rem(m + k, mps) for k in range(1, mps) if k != mps // 2]
    if mps == 4:
        near = [m + 1 - 2 * lax.rem(m, 2), 3 - m]
    plane = [lax.rem(g + k, groups) for k in range(1, groups)]
    serving = plane
    if groups == 4:
        beside = g + 1 - 2 * lax.rem(g, 2)
        serving = [beside, lax.rem(beside + 2, groups), lax.rem(g + 2, groups)]

    barrier = pltpu.get_barrier_semaphore()

    def tell(sem, gg, dd, mm):
        pl.semaphore_signal(sem, inc=1, device_id=(gg, dd, mm), device_id_type=MESH)

    for peer in far:
        tell(barrier, g, d, peer)
    for peer in plane:
        tell(barrier, peer, d, m)
    for e in range(1, depths):
        for k in range(groups):
            tell(barrier, lax.rem(g + k, groups), lax.rem(d + e, depths), m)

    own_columns = pl.ds(pl.multiple_of(m * cols, cols), cols)
    small_pairs = (
        (image_slot_hbm, image_slot),
        (block_list_hbm, block_list),
        (block_count_hbm, block_count),
        (image_first_hbm, image_first),
        (image_count_hbm, image_count),
        (text_length_hbm, text_length),
        (queries_hbm, queries),
        (new_keys_hbm, new_keys),
        (new_values_hbm, new_values),
        (gain_hbm.at[:, own_columns], gain),
        (states_hbm.at[:, own_columns], states_recv.at[m]),
    )
    smalls = [pltpu.make_async_copy(a, b, small_sem.at[i]) for i, (a, b) in enumerate(small_pairs)]
    for small in smalls:
        small.start()
    pairs = (
        (text_keys_hbm, text_keys),
        (text_values_hbm, text_values),
        (image_keys_hbm, image_keys),
        (image_values_hbm, image_values),
        (out_weight_hbm, out_weight),
        (gate_hbm, gate),
        (up_hbm, up),
        (down_hbm, down),
    )
    loads = [pltpu.make_async_copy(a, b, load_sem.at[i]) for i, (a, b) in enumerate(pairs)]
    for i in (0, 2, 3, 1):
        loads[i].start()

    def remote(src, dst, ssem, rsem, gg, dd, mm):
        return pltpu.make_async_remote_copy(
            src_ref=src,
            dst_ref=dst,
            send_sem=ssem,
            recv_sem=rsem,
            device_id=(gg, dd, mm),
            device_id_type=MESH,
        )

    for small in smalls[:6]:
        small.wait()

    own_count = block_count[g]
    counts = [jnp.int32(0)] * (depths * groups)
    for place in range(listed):
        p = place % depths
        owner = lax.div(image_slot[block_list[g, place]], jnp.int32(stored))
        live = (place < own_count).astype(I32)
        rank = jnp.int32(0)
        for o in range(groups):
            mine = owner == o
            rank = jnp.where(mine, counts[p * groups + o], rank)
            counts[p * groups + o] = counts[p * groups + o] + jnp.where(mine, live, 0)
        codes[place] = jnp.minimum(owner * copies + rank, places - 1)

    def wanted(r):
        found = jnp.int32(-1)
        for k in range(READS):
            place = image_first[r] + k
            held = jnp.minimum(place, listed - 1)
            good = (k < image_count[r]) & (place < own_count) & (lax.rem(place, depths) == d)
            found = jnp.where(good, codes[held], found)
        return found

    smalls[6].wait()
    picked = [jnp.zeros((heads, width), F32)] * places
    for r in range(requests):
        code = jnp.full((heads, width), wanted(r), I32)
        q = queries[r].astype(F32)
        picked = [jnp.where(code == i, q, old) for i, old in enumerate(picked)]
    for o in range(groups):
        for c in range(copies):
            query_send[o, c] = picked[o * copies + c].astype(BF16)
    query_recv[g] = query_send[g]

    pl.semaphore_wait(barrier, groups - 1 + (depths - 1) * groups + mps - 1)

    def query_copy(peer, slot):
        return remote(
            query_send.at[peer], query_recv.at[slot], query_ssem, query_rsem.at[slot], peer, d, m
        )

    for peer in plane:
        query_copy(peer, g).start()
    for peer in far:
        tell(ready_sem, g, d, peer)

    def state_copy(peer):
        columns = pl.ds(pl.multiple_of(peer * cols, cols), cols)
        return remote(
            states_hbm.at[:, columns], states_recv.at[m], state_ssem, state_rsem, g, d, peer
        )

    for peer in far:
        state_copy(peer).start()

    def serve_step(i, state):
        place = i * depths + d
        out = []
        for s in range(groups):
            rank, held = state[s]
            slot = image_slot[block_list[s, place]]
            hit = (lax.div(slot, jnp.int32(stored)) == g) & (place < block_count[s])
            within = lax.rem(slot, jnp.int32(stored))
            target = jnp.where(hit, rank, -1)
            held = tuple(jnp.where(target == c, within, old) for c, old in enumerate(held))
            out.append((rank + hit.astype(I32), held))
        return tuple(out)

    zero = jnp.int32(0)
    served = lax.fori_loop(0, steps, serve_step, ((zero, (zero,) * copies),) * groups, unroll=2)
    for s in range(groups):
        for c in range(copies):
            chosen[s * copies + c] = served[s][1][c]

    def by_head(parts):
        result = parts[0]
        row = lax.broadcasted_iota(I32, result.shape, 0)
        for h in range(1, kv_heads):
            result = jnp.where(row >= h * share, parts[h], result)
        return result

    def spread_rows(small):
        return by_head(
            [jnp.broadcast_to(small[h : h + 1, :], (heads, width)) for h in range(kv_heads)]
        )

    def widen(q):
        full = q.astype(F32)
        row = lax.broadcasted_iota(I32, full.shape, 0)
        parts = [
            jnp.where((row >= h * share) & (row < (h + 1) * share), full, 0.0)
            for h in range(kv_heads)
        ]
        return jnp.concatenate(parts, axis=1).astype(BF16)

    def joined(ref, index):
        return jnp.concatenate([ref[index, h] for h in range(kv_heads)], axis=1)

    def split_heads(wide):
        return by_head([wide[:, h * width : (h + 1) * width] for h in range(kv_heads)])

    smalls[7].wait()
    smalls[8].wait()
    loads[0].wait()
    lanes = lax.broadcasted_iota(I32, (heads, span), 1) + d * span

    def text_first(r, carry):
        q = queries[r]
        score = lax.dot_general(widen(q), joined(text_keys, r), NT, preferred_element_type=F32)
        text_scores[r] = jnp.where(lanes < text_length[r], score * scaling, MASKED_SCORE)
        key = spread_rows(new_keys[r].astype(F32))
        new_score = jnp.sum(q.astype(F32) * key, axis=-1, keepdims=True) * scaling
        new_scores[r] = jnp.broadcast_to(new_score, (heads, width))
        return carry

    lax.fori_loop(0, requests, text_first, 0, unroll=True)
    is_first = jnp.full((requests, heads, width), d, I32) == 0
    score = text_scores[...]
    fresh = jnp.where(is_first, new_scores[...], MASKED_SCORE)
    top = jnp.maximum(jnp.max(score, axis=-1, keepdims=True), fresh)
    level = jnp.floor(top / LOG_TWO)
    text_part[:, 1] = level
    weight = jnp.where(
        score > 0.5 * MASKED_SCORE, jnp.exp(score - LOG_TWO * level[:, :, :1]), 0.0
    ).astype(BF16)
    text_weights[...] = weight
    fresh_weight = jnp.where(is_first, jnp.exp(new_scores[...] - LOG_TWO * level), 0.0)
    fresh_weight = fresh_weight.astype(BF16).astype(F32)
    new_scores[...] = fresh_weight
    text_part[:, 2] = jnp.sum(weight.astype(F32), axis=-1, keepdims=True) + fresh_weight
    others = [lax.rem(d + e, depths) for e in range(1, depths)]
    loads[2].wait()
    loads[3].wait()
    for load in loads[4:]:
        load.start()
    stat_lane = lax.broadcasted_iota(I32, (heads, width), 1)
    stat_row = lax.broadcasted_iota(I32, (heads, width), 0)
    own_lane = lax.rem(stat_lane, heads) == stat_row
    stat_kind = lax.div(stat_lane, heads)

    def serve(s):
        slots = [chosen[s * copies + c] for c in range(copies)]
        scores = [
            scaling
            * lax.dot_general(
                widen(query_recv[s, c]),
                joined(image_keys, slots[c]),
                NT,
                preferred_element_type=F32,
            )
            for c in range(copies)
        ]
        stats = jnp.zeros((heads, width), F32)
        weights = []
        for c in range(copies):
            level = jnp.floor(jnp.max(scores[c], axis=-1, keepdims=True) / LOG_TWO)
            weight = jnp.exp(scores[c] - LOG_TWO * level).astype(BF16)
            total = jnp.sum(weight.astype(F32), axis=-1, keepdims=True)
            stats = jnp.where(stat_kind == 2 * c, level, stats)
            stats = jnp.where(stat_kind == 2 * c + 1, total, stats)
            weights.append(weight)
        stat_send[s] = jnp.sum(jnp.where(own_lane, stats, 0.0), axis=0, keepdims=True)
        for c in range(copies):
            wide = jnp.dot(weights[c], joined(image_values, slots[c]), preferred_element_type=F32)
            image_send[s, c] = split_heads(wide).astype(BF16)

    def image_copy(peer, depth):
        return remote(
            image_send.at[peer],
            image_recv.at[pl.ds((d * groups + g) * copies, copies)],
            image_ssem,
            image_rsem,
            peer,
            depth,
            m,
        )

    def stat_copy(peer, depth):
        return remote(
            stat_send.at[peer],
            stat_recv.at[d * groups + g],
            stat_ssem,
            stat_rsem,
            peer,
            depth,
            m,
        )

    serve(g)
    stat_recv[d * groups + g] = stat_send[g]
    image_recv[pl.ds((d * groups + g) * copies, copies)] = image_send[g]
    for other in others:
        image_copy(g, other).start()
        stat_copy(g, other).start()

    loads[1].wait()

    def text_second(r, carry):
        wide = jnp.dot(text_weights[r], joined(text_values, r), preferred_element_type=F32)
        fresh_value = new_scores[r] * spread_rows(new_values[r].astype(F32))
        text_part[r, 0] = split_heads(wide) + fresh_value
        return carry

    lax.fori_loop(0, requests, text_second, 0, unroll=True)

    def text_copy(peer, slot):
        return remote(
            text_part.at[pl.ds(peer * per_depth, per_depth)],
            text_recv.at[slot],
            text_ssem,
            text_rsem.at[slot],
            g,
            peer,
            m,
        )

    for other in others:
        text_copy(other, d).start()
    text_recv[d] = text_part[pl.ds(d * per_depth, per_depth)]

    for s in serving:
        query_copy(s, s).wait_recv()
        serve(s)
        for e in range(depths):
            image_copy(s, lax.rem(d + e, depths)).start()
            stat_copy(s, lax.rem(d + e, depths)).start()

    remote(states_recv.at[pl.ds(0, mps - 1)], states_recv.at[pl.ds(0, mps - 1)], state_ssem, state_rsem, g, d, m).wait_recv()
    smalls[9].wait()
    smalls[10].wait()
    for i in range(mps):
        states_rows[i * rows : (i + 1) * rows, :] = states_recv[i].astype(F32)

    for other in others:
        text_copy(other, other).wait_recv()
    arrivals = depths * groups - 1
    image_all = image_recv.at[pl.ds(0, arrivals * copies)]
    stat_all = stat_recv.at[pl.ds(0, arrivals)]
    remote(stat_all, stat_all, stat_ssem, stat_rsem, g, d, m).wait_recv()
    remote(image_all, image_all, image_ssem, image_rsem, g, d, m).wait_recv()

    def stat_of(stats, lane):
        picked = jnp.sum(jnp.where(stat_lane == lane + stat_row, stats, 0.0), axis=-1, keepdims=True)
        return jnp.broadcast_to(picked, (heads, width))

    def merge(i, carry):
        r = d * per_depth + i
        parts = [tuple(text_recv[e, i, n] for n in range(3)) for e in range(depths)]
        for k in range(READS):
            place = image_first[r] + k
            good = (k < image_count[r]) & (place < own_count)
            held = jnp.minimum(place, listed - 1)
            code = codes[held]
            at = lax.rem(held, depths)
            owner = lax.div(code, jnp.int32(copies))
            rank = lax.rem(code, jnp.int32(copies))
            stats = jnp.broadcast_to(stat_recv[at * groups + owner], (heads, width))
            live = jnp.full((heads, width), good.astype(I32), I32) == 1
            parts.append(
                (
                    jnp.where(live, image_recv[at * places + code].astype(F32), 0.0),
                    jnp.where(live, stat_of(stats, 2 * rank * heads), MASKED_SCORE),
                    jnp.where(live, stat_of(stats, (2 * rank + 1) * heads), 0.0),
                )
            )
        highest = functools.reduce(jnp.maximum, [part[1] for part in parts])
        factors = [jnp.exp2(part[1] - highest) for part in parts]
        total = sum(part[2] * factor for part, factor in zip(parts, factors))
        value = sum(part[0] * factor for part, factor in zip(parts, factors)) / total
        merged[i] = value
        attention_out[i] = value.astype(BF16)
        return carry

    lax.fori_loop(0, per_depth, merge, 0, unroll=True)
    for h in range(heads):
        flat[:, h * width : (h + 1) * width] = merged[:, h, :]

    loads[4].wait()
    low = flat[...].astype(BF16)

    def project(block):
        columns = pl.ds(pl.multiple_of(block * cols, cols), cols)
        return jnp.dot(low, out_weight[:, columns], preferred_element_type=F32)

    def proj_copy(k, peer):
        return remote(proj_send.at[k], proj_recv.at[m], proj_ssem, proj_rsem, g, d, peer)

    ahead = project(far[0])
    for k, peer in enumerate(far):
        block = ahead
        ahead = project((far + [m])[k + 1])
        proj_send[k] = block.astype(BF16)
        proj_copy(k, peer).start()
    total = ahead + states_rows[...]
    sent = proj_send.at[pl.ds(0, mps - 1)]
    remote(sent, proj_recv.at[pl.ds(0, mps - 1)], proj_ssem, proj_rsem, g, d, m).wait_recv()
    for k in range(1, mps):
        total = total + proj_recv[lax.rem(m + k, mps)].astype(F32)
    res_cols[...] = total
    me = m * groups + g
    x_all[me] = (total * gain[...]).astype(BF16)
    square = jnp.broadcast_to(jnp.sum(total * total, axis=-1, keepdims=True), (per_depth, width))
    square_lane = lax.broadcasted_iota(I32, (per_depth, width), 1)
    square_row = lax.broadcasted_iota(I32, (per_depth, width), 0)
    diagonal = square_lane == square_row
    square_cols[m] = jnp.sum(jnp.where(diagonal, square, 0.0), axis=0, keepdims=True)

    pl.semaphore_wait(ready_sem, mps - 1)

    def x_copy(gg, mm):
        return remote(x_all.at[me], x_all.at[me], x_ssem, x_rsem.at[m], gg, d, mm)

    def column_copy(peer):
        return remote(
            square_cols.at[m], square_cols.at[m], square_ssem.at[0], square_rsem.at[0], g, d, peer
        )

    def square_copy(peer):
        return remote(
            square_all.at[g], square_all.at[g], square_ssem.at[1], square_rsem.at[1], peer, d, m
        )

    ring = [lax.rem(g * mps + m + k, pieces) for k in range(1, pieces)]
    targets = [(lax.div(p, mps), lax.rem(p, mps)) for p in ring]
    relayed = lax.rem(m + mps // 2, mps)
    handed = relayed * groups + g

    def hand_copy():
        return remote(x_all.at[me], x_all.at[me], x_ssem, hand_rsem, g, d, relayed)

    def pass_copy(peer):
        return remote(
            x_all.at[handed], x_all.at[handed], x_ssem, x_rsem.at[relayed], peer, d, m
        )

    hand_copy().start()
    for peer in far:
        column_copy(peer).start()
    for k, (gg, mm) in enumerate(targets):
        if (k + 1) % mps != mps // 2:
            x_copy(gg, mm).start()

    for i in range(mps):
        res_send[i] = res_cols[i * rows : (i + 1) * rows, :]

    def res_copy(peer):
        return remote(res_send.at[peer], res_recv.at[m], res_ssem, res_rsem, g, d, peer)


    loads[5].wait()
    loads[6].wait()
    loads[7].wait()

    def expand(block, first):
        tokens = [x_all[block * groups + s].astype(F32) for s in range(groups)]
        tokens = jnp.concatenate(tokens, axis=0).astype(BF16)
        part = pl.ds(pl.multiple_of(block * cols, cols), cols)
        a = jnp.dot(tokens, gate[part, :], preferred_element_type=F32)
        b = jnp.dot(tokens, up[part, :], preferred_element_type=F32)
        if first:
            gate_sum[...] = a
            up_sum[...] = b
        else:
            gate_sum[...] += a
            up_sum[...] += b

    def x_wait(block, count):
        got = x_all.at[pl.ds(0, count)]
        remote(got, got, x_ssem, x_rsem.at[block], g, d, m).wait_recv()

    remote(x_all.at[0], x_all.at[0], x_ssem, hand_rsem, g, d, m).wait_recv()
    for peer in plane:
        pass_copy(peer).start()
    got = square_cols.at[pl.ds(0, mps - 1)]
    remote(got, got, square_ssem.at[0], square_rsem.at[0], g, d, m).wait_recv()
    square_all[g] = sum(square_cols[i] for i in range(mps))
    for peer in plane:
        square_copy(peer).start()

    x_wait(m, groups - 1)
    expand(m, True)
    for block in near:
        x_wait(block, groups)
        expand(block, False)
    got = square_all.at[pl.ds(0, groups - 1)]
    remote(got, got, square_ssem.at[1], square_rsem.at[1], g, d, m).wait_recv()
    scales = []
    for s in range(groups):
        row = jnp.broadcast_to(square_all[s], (per_depth, width))
        mean = jnp.sum(jnp.where(diagonal, row, 0.0), axis=-1, keepdims=True) / model
        scales.append(lax.rsqrt(mean + NORM_EPSILON))
    scale = jnp.concatenate(scales, axis=0)
    x_wait(relayed, groups - 1)
    expand(relayed, False)
    for peer in far:
        res_copy(peer).start()
    res_recv[m] = res_send[m]
    v = gate_sum[...] * scale
    hidden[...] = (v / (1.0 + jnp.exp(-v)) * (up_sum[...] * scale)).astype(BF16)

    def down_copy(n, gg, mm):
        return remote(
            down_send.at[n, mm * groups + gg],
            down_recv.at[me, n],
            down_ssem,
            down_rsem,
            gg,
            d,
            mm,
        )

    for n in range(chunks):
        columns = slice(n * part_cols, (n + 1) * part_cols)
        part = jnp.dot(hidden[...], down[:, columns], preferred_element_type=F32)
        for s in range(groups):
            for i in range(mps):
                at = s * per_depth + i * rows
                down_send[n, i * groups + s] = part[at : at + rows, :].astype(BF16)
        for gg, mm in targets:
            down_copy(n, gg, mm).start()
    down_recv[me] = down_send[:, me]

    got = res_recv.at[pl.ds(0, mps - 1)]
    remote(got, got, res_ssem, res_rsem, g, d, m).wait_recv()
    got = down_recv.at[pl.ds(0, pieces - 1)]
    remote(got, got, down_ssem, down_rsem, g, d, m).wait_recv()

    for n in range(chunks):

        def add_piece(i, total):
            return total + down_recv[i, n].astype(F32)

        summed = lax.fori_loop(0, pieces, add_piece, jnp.zeros((rows, part_cols), F32), unroll=4)
        for i in range(mps):
            low_edge, high_edge = max(n * part_cols, i * cols), min((n + 1) * part_cols, (i + 1) * cols)
            if low_edge < high_edge:
                layer_out[:, low_edge:high_edge] = (
                    summed[:, low_edge - n * part_cols : high_edge - n * part_cols]
                    + res_recv[i, :, low_edge - i * cols : high_edge - i * cols]
                ).astype(BF16)

    def sent_all(ref, ssem, rsem):
        remote(ref, ref, ssem, rsem, g, d, m).wait_send()

    sent_all(states_recv.at[pl.ds(0, mps - 1)], state_ssem, state_rsem)
    sent_all(query_send.at[pl.ds(0, groups - 1)], query_ssem, query_rsem.at[0])
    for other in others:
        text_copy(other, d).wait_send()
    sent_all(image_all, image_ssem, image_rsem)
    sent_all(stat_all, stat_ssem, stat_rsem)
    sent_all(proj_send.at[pl.ds(0, mps - 1)], proj_ssem, proj_rsem)
    sent_all(x_all.at[pl.ds(0, pieces - 1)], x_ssem, x_rsem.at[0])
    sent_all(square_cols.at[pl.ds(0, mps - 1)], square_ssem.at[0], square_rsem.at[0])
    sent_all(square_all.at[pl.ds(0, groups - 1)], square_ssem.at[1], square_rsem.at[1])
    sent_all(res_send.at[pl.ds(0, mps - 1)], res_ssem, res_rsem)
    sent_all(down_recv.at[pl.ds(0, pieces - 1)], down_ssem, down_rsem)


def finish(attention, layer, attention_out, layer_out):
    attention_out[...] = attention[...]
    layer_out[...] = layer[...]


def on_device(
    states,
    queries,
    new_keys,
    new_values,
    text_keys,
    text_values,
    text_length,
    image_keys,
    image_values,
    image_slot,
    block_list,
    block_count,
    image_first,
    image_count,
    out_weight,
    norm_gain,
    gate_weight,
    up_weight,
    down_weight,
):
    groups = lax.axis_size("group")
    depths = lax.axis_size("depth")
    mps = lax.axis_size("mp")
    pieces = groups * mps
    requests, heads, width = queries.shape
    listed = block_list.shape[1]
    copies = listed // (depths * groups)
    per_depth = requests // depths
    rows, model = states.shape
    cols = model // mps
    units = gate_weight.shape[1]
    span = text_keys.shape[2]
    part_cols = model // DOWN_CHUNKS
    dma = pltpu.SemaphoreType.DMA
    vmem = pl.BlockSpec(memory_space=pltpu.VMEM)
    hbm = pl.BlockSpec(memory_space=pl.ANY)
    small = (
        states,
        queries,
        new_keys,
        new_values,
        norm_gain.reshape(1, model),
        text_length,
        image_slot,
        block_list,
        block_count,
        image_first,
        image_count,
    )
    big = (
        text_keys,
        text_values,
        image_keys,
        image_values,
        out_weight,
        gate_weight,
        up_weight,
        down_weight,
    )
    scratch = [pltpu.VMEM(a.shape, a.dtype) for a in small[1:4]]
    scratch += [pltpu.VMEM((1, cols), norm_gain.dtype)]
    scratch += [pltpu.SMEM(a.shape, a.dtype) for a in small[5:]]
    scratch += [pltpu.VMEM(a.shape, a.dtype) for a in big]
    scratch += [
        pltpu.SMEM((groups * copies,), I32),
        pltpu.SMEM((listed,), I32),
        pltpu.VMEM((mps, rows, cols), BF16),
        pltpu.VMEM((groups, copies, heads, width), BF16),
        pltpu.VMEM((groups, copies, heads, width), BF16),
        pltpu.VMEM((requests, heads, span), F32),
        pltpu.VMEM((requests, heads, width), F32),
        pltpu.VMEM((requests, heads, span), BF16),
        pltpu.VMEM((requests, 3, heads, width), F32),
        pltpu.VMEM((depths, per_depth, 3, heads, width), F32),
        pltpu.VMEM((groups, copies, heads, width), BF16),
        pltpu.VMEM((groups, 1, width), F32),
        pltpu.VMEM((depths * groups * copies, heads, width), BF16),
        pltpu.VMEM((depths * groups, 1, width), F32),
        pltpu.VMEM((per_depth, heads, width), F32),
        pltpu.VMEM((per_depth, heads * width), F32),
        pltpu.VMEM((mps, per_depth, cols), BF16),
        pltpu.VMEM((mps, per_depth, cols), BF16),
        pltpu.VMEM((per_depth, cols), F32),
        pltpu.VMEM((per_depth, cols), F32),
        pltpu.VMEM((mps, rows, cols), F32),
        pltpu.VMEM((mps, rows, cols), F32),
        pltpu.VMEM((pieces, per_depth, cols), BF16),
        pltpu.VMEM((mps, 1, width), F32),
        pltpu.VMEM((groups, 1, width), F32),
        pltpu.VMEM((groups * per_depth, units), F32),
        pltpu.VMEM((groups * per_depth, units), F32),
        pltpu.VMEM((groups * per_depth, units), BF16),
        pltpu.VMEM((DOWN_CHUNKS, pieces, rows, part_cols), BF16),
        pltpu.VMEM((pieces, DOWN_CHUNKS, rows, part_cols), BF16),
        dma((len(big),)),
        dma((len(small),)),
        dma,
        dma,
        dma,
        dma((groups,)),
        dma,
        dma((depths,)),
        dma,
        dma,
        dma,
        dma,
        dma,
        dma,
        dma,
        dma((mps,)),
        dma,
        dma((2,)),
        dma((2,)),
        dma,
        dma,
        dma,
        dma,
        pltpu.SemaphoreType.REGULAR,
    ]
    raw = pl.pallas_call(
        functools.partial(kernel, (groups, depths, mps)),
        out_shape=(
            pltpu.VMEM((per_depth, heads, width), BF16),
            pltpu.VMEM((rows, model), BF16),
        ),
        in_specs=[hbm] * 19,
        out_specs=(vmem, vmem),
        scratch_shapes=scratch,
        compiler_params=pltpu.CompilerParams(
            collective_id=0, has_side_effects=True, vmem_limit_bytes=60000000
        ),
    )(*small, *big)
    return pl.pallas_call(
        finish,
        out_shape=(
            jax.ShapeDtypeStruct((per_depth, heads, width), BF16),
            jax.ShapeDtypeStruct((rows, model), BF16),
        ),
        in_specs=[vmem] * 2,
        out_specs=(vmem, vmem),
    )(*(pltpu.with_memory_space_constraint(r, pltpu.VMEM) for r in raw))


def solution(mesh):
    placed = (
        P(("group", "depth", "mp"), None),
        P("group", "mp", None),
        P("group", "mp", None),
        P("group", "mp", None),
        P("group", "mp", "depth", None),
        P("group", "mp", "depth", None),
        P("group"),
        P("group", "mp", None, None),
        P("group", "mp", None, None),
        P(),
        P(),
        P(),
        P("group"),
        P("group"),
        P("mp", None),
        P(),
        P(None, ("group", "mp")),
        P(None, ("group", "mp")),
        P(("group", "mp"), None),
    )
    return jax.shard_map(
        on_device,
        mesh=mesh,
        in_specs=placed,
        out_specs=(P(("group", "depth"), "mp", None), P(("group", "depth", "mp"), None)),
        check_vma=False,
    )
```

```python
import functools
import math

import jax
import jax.numpy as jnp
from jax import lax
from jax.experimental import pallas as pl
from jax.experimental.pallas import tpu as pltpu
from jax.sharding import PartitionSpec as P

LOG_TWO = math.log(2.0)
MASKED_SCORE = -1e30
NORM_EPSILON = 1e-05
READS = 2
DOWN_CHUNKS = 1
MESH = pl.DeviceIdType.MESH
F32 = jnp.float32
BF16 = jnp.bfloat16
I32 = jnp.int32
NT = (((1,), (1,)), ((), ()))


def kernel(
    dims,
    states_hbm,
    queries_hbm,
    new_keys_hbm,
    new_values_hbm,
    gain_hbm,
    text_length_hbm,
    image_slot_hbm,
    block_list_hbm,
    block_count_hbm,
    image_first_hbm,
    image_count_hbm,
    text_keys_hbm,
    text_values_hbm,
    image_keys_hbm,
    image_values_hbm,
    out_weight_hbm,
    gate_hbm,
    up_hbm,
    down_hbm,
    attention_out,
    layer_out,
    queries,
    new_keys,
    new_values,
    gain,
    text_length,
    image_slot,
    block_list,
    block_count,
    image_first,
    image_count,
    text_keys,
    text_values,
    image_keys,
    image_values,
    out_weight,
    gate,
    up,
    down,
    chosen,
    codes,
    states_recv,
    query_send,
    query_recv,
    text_scores,
    new_scores,
    text_weights,
    text_part,
    text_recv,
    image_send,
    stat_send,
    image_recv,
    stat_recv,
    merged,
    flat,
    proj_send,
    proj_recv,
    states_rows,
    res_cols,
    res_send,
    res_recv,
    x_all,
    square_sum,
    gate_sum,
    up_sum,
    hidden,
    down_send,
    down_recv,
    load_sem,
    small_sem,
    state_ssem,
    state_rsem,
    query_ssem,
    query_rsem,
    text_ssem,
    text_rsem,
    image_ssem,
    image_rsem,
    stat_ssem,
    stat_rsem,
    proj_ssem,
    proj_rsem,
    x_ssem,
    x_rsem,
    hand_rsem,
    res_ssem,
    res_rsem,
    down_ssem,
    down_rsem,
    ready_sem,
):
    groups, depths, mps = dims
    pieces = groups * mps
    g = lax.axis_index("group")
    d = lax.axis_index("depth")
    m = lax.axis_index("mp")
    requests, heads, width = queries.shape
    kv_heads, span = text_keys.shape[1], text_keys.shape[2]
    share = heads // kv_heads
    stored, patches = image_keys.shape[0], image_keys.shape[2]
    listed = block_list.shape[1]
    steps = listed // depths
    copies = listed // (depths * groups)
    places = groups * copies
    per_depth = requests // depths
    rows = states_recv.shape[1]
    model = layer_out.shape[1]
    cols = model // mps
    chunks, part_cols = down_recv.shape[1], down_recv.shape[3]
    scaling = 1.0 / math.sqrt(width)
    far = [lax.rem(m + k, mps) for k in range(1, mps)]
    if mps % 2 == 0:
        half = lax.div(m, mps // 2)
        far = [
            (1 - half) * (mps - 1 - k - lax.div(m + k, mps - 1))
            + half * (k + lax.div(mps - 1 + k - m, mps - 1))
            for k in range(mps - 1)
        ]
    near = [lax.rem(m + k, mps) for k in range(1, mps) if k != mps // 2]
    if mps == 4:
        near = [m + 1 - 2 * lax.rem(m, 2), 3 - m]
    plane = [lax.rem(g + k, groups) for k in range(1, groups)]
    serving = plane
    if groups == 4:
        beside = g + 1 - 2 * lax.rem(g, 2)
        serving = [beside, lax.rem(beside + 2, groups), lax.rem(g + 2, groups)]

    barrier = pltpu.get_barrier_semaphore()

    def tell(sem, gg, dd, mm):
        pl.semaphore_signal(sem, inc=1, device_id=(gg, dd, mm), device_id_type=MESH)

    for peer in far:
        tell(barrier, g, d, peer)
    for peer in plane:
        tell(barrier, peer, d, m)
    for e in range(1, depths):
        for k in range(groups):
            tell(barrier, lax.rem(g + k, groups), lax.rem(d + e, depths), m)

    own_columns = pl.ds(pl.multiple_of(m * cols, cols), cols)
    small_pairs = (
        (image_slot_hbm, image_slot),
        (block_list_hbm, block_list),
        (block_count_hbm, block_count),
        (image_first_hbm, image_first),
        (image_count_hbm, image_count),
        (text_length_hbm, text_length),
        (queries_hbm, queries),
        (new_keys_hbm, new_keys),
        (new_values_hbm, new_values),
        (gain_hbm, gain),
        (states_hbm.at[:, own_columns], states_recv.at[m]),
    )
    smalls = [pltpu.make_async_copy(a, b, small_sem.at[i]) for i, (a, b) in enumerate(small_pairs)]
    for small in smalls:
        small.start()
    pairs = (
        (text_keys_hbm, text_keys),
        (text_values_hbm, text_values),
        (image_keys_hbm, image_keys),
        (image_values_hbm, image_values),
        (out_weight_hbm, out_weight),
        (gate_hbm, gate),
        (up_hbm, up),
        (down_hbm, down),
    )
    loads = [pltpu.make_async_copy(a, b, load_sem.at[i]) for i, (a, b) in enumerate(pairs)]
    for i in (0, 2, 3, 1):
        loads[i].start()

    def remote(src, dst, ssem, rsem, gg, dd, mm):
        return pltpu.make_async_remote_copy(
            src_ref=src,
            dst_ref=dst,
            send_sem=ssem,
            recv_sem=rsem,
            device_id=(gg, dd, mm),
            device_id_type=MESH,
        )

    for small in smalls[:6]:
        small.wait()

    own_count = block_count[g]
    counts = [jnp.int32(0)] * (depths * groups)
    for place in range(listed):
        p = place % depths
        owner = lax.div(image_slot[block_list[g, place]], jnp.int32(stored))
        live = (place < own_count).astype(I32)
        rank = jnp.int32(0)
        for o in range(groups):
            mine = owner == o
            rank = jnp.where(mine, counts[p * groups + o], rank)
            counts[p * groups + o] = counts[p * groups + o] + jnp.where(mine, live, 0)
        codes[place] = jnp.minimum(owner * copies + rank, places - 1)

    def wanted(r):
        found = jnp.int32(-1)
        for k in range(READS):
            place = image_first[r] + k
            held = jnp.minimum(place, listed - 1)
            good = (k < image_count[r]) & (place < own_count) & (lax.rem(place, depths) == d)
            found = jnp.where(good, codes[held], found)
        return found

    smalls[6].wait()
    picked = [jnp.zeros((heads, width), F32)] * places
    for r in range(requests):
        code = jnp.full((heads, width), wanted(r), I32)
        q = queries[r].astype(F32)
        picked = [jnp.where(code == i, q, old) for i, old in enumerate(picked)]
    for o in range(groups):
        for c in range(copies):
            query_send[o, c] = picked[o * copies + c].astype(BF16)
    query_recv[g] = query_send[g]

    pl.semaphore_wait(barrier, groups - 1 + (depths - 1) * groups + mps - 1)

    def query_copy(peer, slot):
        return remote(
            query_send.at[peer], query_recv.at[slot], query_ssem, query_rsem.at[slot], peer, d, m
        )

    for peer in plane:
        query_copy(peer, g).start()
    for peer in far:
        tell(ready_sem, g, d, peer)

    def state_copy(peer):
        columns = pl.ds(pl.multiple_of(peer * cols, cols), cols)
        return remote(
            states_hbm.at[:, columns], states_recv.at[m], state_ssem, state_rsem, g, d, peer
        )

    for peer in far:
        state_copy(peer).start()

    def serve_step(i, state):
        place = i * depths + d
        out = []
        for s in range(groups):
            rank, held = state[s]
            slot = image_slot[block_list[s, place]]
            hit = (lax.div(slot, jnp.int32(stored)) == g) & (place < block_count[s])
            within = lax.rem(slot, jnp.int32(stored))
            target = jnp.where(hit, rank, -1)
            held = tuple(jnp.where(target == c, within, old) for c, old in enumerate(held))
            out.append((rank + hit.astype(I32), held))
        return tuple(out)

    zero = jnp.int32(0)
    served = lax.fori_loop(0, steps, serve_step, ((zero, (zero,) * copies),) * groups, unroll=2)
    for s in range(groups):
        for c in range(copies):
            chosen[s * copies + c] = served[s][1][c]

    def by_head(parts):
        result = parts[0]
        row = lax.broadcasted_iota(I32, result.shape, 0)
        for h in range(1, kv_heads):
            result = jnp.where(row >= h * share, parts[h], result)
        return result

    def spread_rows(small):
        return by_head(
            [jnp.broadcast_to(small[h : h + 1, :], (heads, width)) for h in range(kv_heads)]
        )

    def widen(q):
        full = q.astype(F32)
        row = lax.broadcasted_iota(I32, full.shape, 0)
        parts = [
            jnp.where((row >= h * share) & (row < (h + 1) * share), full, 0.0)
            for h in range(kv_heads)
        ]
        return jnp.concatenate(parts, axis=1).astype(BF16)

    def joined(ref, index):
        return jnp.concatenate([ref[index, h] for h in range(kv_heads)], axis=1)

    def split_heads(wide):
        return by_head([wide[:, h * width : (h + 1) * width] for h in range(kv_heads)])

    smalls[7].wait()
    smalls[8].wait()
    loads[0].wait()
    lanes = lax.broadcasted_iota(I32, (heads, span), 1) + d * span

    def text_first(r, carry):
        q = queries[r]
        score = lax.dot_general(widen(q), joined(text_keys, r), NT, preferred_element_type=F32)
        text_scores[r] = jnp.where(lanes < text_length[r], score * scaling, MASKED_SCORE)
        key = spread_rows(new_keys[r].astype(F32))
        new_score = jnp.sum(q.astype(F32) * key, axis=-1, keepdims=True) * scaling
        new_scores[r] = jnp.broadcast_to(new_score, (heads, width))
        return carry

    lax.fori_loop(0, requests, text_first, 0, unroll=True)
    is_first = jnp.full((requests, heads, width), d, I32) == 0
    score = text_scores[...]
    fresh = jnp.where(is_first, new_scores[...], MASKED_SCORE)
    top = jnp.maximum(jnp.max(score, axis=-1, keepdims=True), fresh)
    level = jnp.floor(top / LOG_TWO)
    text_part[:, 1] = level
    weight = jnp.where(
        score > 0.5 * MASKED_SCORE, jnp.exp(score - LOG_TWO * level[:, :, :1]), 0.0
    ).astype(BF16)
    text_weights[...] = weight
    fresh_weight = jnp.where(is_first, jnp.exp(new_scores[...] - LOG_TWO * level), 0.0)
    fresh_weight = fresh_weight.astype(BF16).astype(F32)
    new_scores[...] = fresh_weight
    text_part[:, 2] = jnp.sum(weight.astype(F32), axis=-1, keepdims=True) + fresh_weight
    others = [lax.rem(d + e, depths) for e in range(1, depths)]
    loads[2].wait()
    loads[3].wait()
    for load in loads[4:]:
        load.start()
    stat_lane = lax.broadcasted_iota(I32, (heads, width), 1)
    stat_row = lax.broadcasted_iota(I32, (heads, width), 0)
    own_lane = lax.rem(stat_lane, heads) == stat_row
    stat_kind = lax.div(stat_lane, heads)

    def serve(s):
        slots = [chosen[s * copies + c] for c in range(copies)]
        scores = [
            scaling
            * lax.dot_general(
                widen(query_recv[s, c]),
                joined(image_keys, slots[c]),
                NT,
                preferred_element_type=F32,
            )
            for c in range(copies)
        ]
        stats = jnp.zeros((heads, width), F32)
        weights = []
        for c in range(copies):
            level = jnp.floor(jnp.max(scores[c], axis=-1, keepdims=True) / LOG_TWO)
            weight = jnp.exp(scores[c] - LOG_TWO * level).astype(BF16)
            total = jnp.sum(weight.astype(F32), axis=-1, keepdims=True)
            stats = jnp.where(stat_kind == 2 * c, level, stats)
            stats = jnp.where(stat_kind == 2 * c + 1, total, stats)
            weights.append(weight)
        stat_send[s] = jnp.sum(jnp.where(own_lane, stats, 0.0), axis=0, keepdims=True)
        for c in range(copies):
            wide = jnp.dot(weights[c], joined(image_values, slots[c]), preferred_element_type=F32)
            image_send[s, c] = split_heads(wide).astype(BF16)

    def image_copy(peer, depth):
        return remote(
            image_send.at[peer],
            image_recv.at[pl.ds((d * groups + g) * copies, copies)],
            image_ssem,
            image_rsem,
            peer,
            depth,
            m,
        )

    def stat_copy(peer, depth):
        return remote(
            stat_send.at[peer],
            stat_recv.at[d * groups + g],
            stat_ssem,
            stat_rsem,
            peer,
            depth,
            m,
        )

    serve(g)
    stat_recv[d * groups + g] = stat_send[g]
    image_recv[pl.ds((d * groups + g) * copies, copies)] = image_send[g]
    for other in others:
        image_copy(g, other).start()
        stat_copy(g, other).start()

    loads[1].wait()

    def text_second(r, carry):
        wide = jnp.dot(text_weights[r], joined(text_values, r), preferred_element_type=F32)
        fresh_value = new_scores[r] * spread_rows(new_values[r].astype(F32))
        text_part[r, 0] = split_heads(wide) + fresh_value
        return carry

    lax.fori_loop(0, requests, text_second, 0, unroll=True)

    def text_copy(peer, slot):
        return remote(
            text_part.at[pl.ds(peer * per_depth, per_depth)],
            text_recv.at[slot],
            text_ssem,
            text_rsem.at[slot],
            g,
            peer,
            m,
        )

    for other in others:
        text_copy(other, d).start()
    text_recv[d] = text_part[pl.ds(d * per_depth, per_depth)]

    for s in serving:
        query_copy(s, s).wait_recv()
        serve(s)
        for e in range(depths):
            image_copy(s, lax.rem(d + e, depths)).start()
            stat_copy(s, lax.rem(d + e, depths)).start()

    remote(states_recv.at[pl.ds(0, mps - 1)], states_recv.at[pl.ds(0, mps - 1)], state_ssem, state_rsem, g, d, m).wait_recv()
    smalls[9].wait()
    smalls[10].wait()
    for i in range(mps):
        states_rows[i * rows : (i + 1) * rows, :] = states_recv[i].astype(F32)

    for other in others:
        text_copy(other, other).wait_recv()
    arrivals = depths * groups - 1
    image_all = image_recv.at[pl.ds(0, arrivals * copies)]
    stat_all = stat_recv.at[pl.ds(0, arrivals)]
    remote(stat_all, stat_all, stat_ssem, stat_rsem, g, d, m).wait_recv()
    remote(image_all, image_all, image_ssem, image_rsem, g, d, m).wait_recv()

    def stat_of(stats, lane):
        picked = jnp.sum(jnp.where(stat_lane == lane + stat_row, stats, 0.0), axis=-1, keepdims=True)
        return jnp.broadcast_to(picked, (heads, width))

    def merge(i, carry):
        r = d * per_depth + i
        parts = [tuple(text_recv[e, i, n] for n in range(3)) for e in range(depths)]
        for k in range(READS):
            place = image_first[r] + k
            good = (k < image_count[r]) & (place < own_count)
            held = jnp.minimum(place, listed - 1)
            code = codes[held]
            at = lax.rem(held, depths)
            owner = lax.div(code, jnp.int32(copies))
            rank = lax.rem(code, jnp.int32(copies))
            stats = jnp.broadcast_to(stat_recv[at * groups + owner], (heads, width))
            live = jnp.full((heads, width), good.astype(I32), I32) == 1
            parts.append(
                (
                    jnp.where(live, image_recv[at * places + code].astype(F32), 0.0),
                    jnp.where(live, stat_of(stats, 2 * rank * heads), MASKED_SCORE),
                    jnp.where(live, stat_of(stats, (2 * rank + 1) * heads), 0.0),
                )
            )
        highest = functools.reduce(jnp.maximum, [part[1] for part in parts])
        factors = [jnp.exp2(part[1] - highest) for part in parts]
        total = sum(part[2] * factor for part, factor in zip(parts, factors))
        value = sum(part[0] * factor for part, factor in zip(parts, factors)) / total
        merged[i] = value
        attention_out[i] = value.astype(BF16)
        return carry

    lax.fori_loop(0, per_depth, merge, 0, unroll=True)
    for h in range(heads):
        flat[:, h * width : (h + 1) * width] = merged[:, h, :]

    loads[4].wait()
    low = flat[...].astype(BF16)

    def project(block):
        columns = pl.ds(pl.multiple_of(block * cols, cols), cols)
        return jnp.dot(low, out_weight[:, columns], preferred_element_type=F32)

    def proj_copy(k, peer):
        return remote(proj_send.at[k], proj_recv.at[m], proj_ssem, proj_rsem, g, d, peer)

    ahead = project(far[0])
    for k, peer in enumerate(far):
        block = ahead
        ahead = project((far + [m])[k + 1])
        proj_send[k] = block.astype(BF16)
        proj_copy(k, peer).start()
    total = ahead + states_rows[...]
    sent = proj_send.at[pl.ds(0, mps - 1)]
    remote(sent, proj_recv.at[pl.ds(0, mps - 1)], proj_ssem, proj_rsem, g, d, m).wait_recv()
    for k in range(1, mps):
        total = total + proj_recv[lax.rem(m + k, mps)].astype(F32)
    res_cols[...] = total
    me = m * groups + g
    x_all[me] = (total * gain[:, own_columns]).astype(BF16)

    pl.semaphore_wait(ready_sem, mps - 1)

    def x_copy(gg, mm):
        return remote(x_all.at[me], x_all.at[me], x_ssem, x_rsem.at[m], gg, d, mm)

    ring = [lax.rem(g * mps + m + k, pieces) for k in range(1, pieces)]
    targets = [(lax.div(p, mps), lax.rem(p, mps)) for p in ring]
    relayed = lax.rem(m + mps // 2, mps)
    handed = relayed * groups + g

    def hand_copy():
        return remote(x_all.at[me], x_all.at[me], x_ssem, hand_rsem, g, d, relayed)

    def pass_copy(peer):
        return remote(
            x_all.at[handed], x_all.at[handed], x_ssem, x_rsem.at[relayed], peer, d, m
        )

    hand_copy().start()
    for k, (gg, mm) in enumerate(targets):
        if (k + 1) % mps != mps // 2:
            x_copy(gg, mm).start()

    for i in range(mps):
        res_send[i] = res_cols[i * rows : (i + 1) * rows, :]

    def res_copy(peer):
        return remote(res_send.at[peer], res_recv.at[m], res_ssem, res_rsem, g, d, peer)


    loads[5].wait()
    loads[6].wait()
    loads[7].wait()

    def expand(block, first):
        tokens = [x_all[block * groups + s].astype(F32) for s in range(groups)]
        tokens = jnp.concatenate(tokens, axis=0)
        part = pl.ds(pl.multiple_of(block * cols, cols), cols)
        plain = tokens * (1.0 / gain[:, part])
        squares = sum(
            plain[:, i : i + width] * plain[:, i : i + width] for i in range(0, cols, width)
        )
        tokens = tokens.astype(BF16)
        a = jnp.dot(tokens, gate[part, :], preferred_element_type=F32)
        b = jnp.dot(tokens, up[part, :], preferred_element_type=F32)
        if first:
            gate_sum[...] = a
            up_sum[...] = b
            square_sum[...] = squares
        else:
            gate_sum[...] += a
            up_sum[...] += b
            square_sum[...] += squares

    def x_wait(block, count):
        got = x_all.at[pl.ds(0, count)]
        remote(got, got, x_ssem, x_rsem.at[block], g, d, m).wait_recv()

    remote(x_all.at[0], x_all.at[0], x_ssem, hand_rsem, g, d, m).wait_recv()
    for peer in plane:
        pass_copy(peer).start()
    x_wait(m, groups - 1)
    expand(m, True)
    for block in near:
        x_wait(block, groups)
        expand(block, False)
    x_wait(relayed, groups - 1)
    expand(relayed, False)
    for peer in far:
        res_copy(peer).start()
    res_recv[m] = res_send[m]
    spread = jnp.sum(square_sum[...], axis=-1, keepdims=True) / model
    scale = lax.rsqrt(spread + NORM_EPSILON)
    v = gate_sum[...] * scale
    hidden[...] = (v / (1.0 + jnp.exp(-v)) * (up_sum[...] * scale)).astype(BF16)

    def down_copy(n, gg, mm):
        return remote(
            down_send.at[n, mm * groups + gg],
            down_recv.at[me, n],
            down_ssem,
            down_rsem,
            gg,
            d,
            mm,
        )

    for n in range(chunks):
        columns = slice(n * part_cols, (n + 1) * part_cols)
        part = jnp.dot(hidden[...], down[:, columns], preferred_element_type=F32)
        for s in range(groups):
            for i in range(mps):
                at = s * per_depth + i * rows
                down_send[n, i * groups + s] = part[at : at + rows, :].astype(BF16)
        for shift in [mps // 2] + [k for k in range(mps) if k != mps // 2]:
            for k, (gg, mm) in enumerate(targets):
                if (k + 1) % mps == shift:
                    down_copy(n, gg, mm).start()
    down_recv[me] = down_send[:, me]

    got = res_recv.at[pl.ds(0, mps - 1)]
    remote(got, got, res_ssem, res_rsem, g, d, m).wait_recv()
    got = down_recv.at[pl.ds(0, pieces - 1)]
    remote(got, got, down_ssem, down_rsem, g, d, m).wait_recv()

    for n in range(chunks):

        def add_piece(i, total):
            return total + down_recv[i, n].astype(F32)

        summed = lax.fori_loop(0, pieces, add_piece, jnp.zeros((rows, part_cols), F32), unroll=4)
        for i in range(mps):
            low_edge, high_edge = max(n * part_cols, i * cols), min((n + 1) * part_cols, (i + 1) * cols)
            if low_edge < high_edge:
                layer_out[:, low_edge:high_edge] = (
                    summed[:, low_edge - n * part_cols : high_edge - n * part_cols]
                    + res_recv[i, :, low_edge - i * cols : high_edge - i * cols]
                ).astype(BF16)

    def sent_all(ref, ssem, rsem):
        remote(ref, ref, ssem, rsem, g, d, m).wait_send()

    sent_all(states_recv.at[pl.ds(0, mps - 1)], state_ssem, state_rsem)
    sent_all(query_send.at[pl.ds(0, groups - 1)], query_ssem, query_rsem.at[0])
    for other in others:
        text_copy(other, d).wait_send()
    sent_all(image_all, image_ssem, image_rsem)
    sent_all(stat_all, stat_ssem, stat_rsem)
    sent_all(proj_send.at[pl.ds(0, mps - 1)], proj_ssem, proj_rsem)
    sent_all(x_all.at[pl.ds(0, pieces - 1)], x_ssem, x_rsem.at[0])
    sent_all(res_send.at[pl.ds(0, mps - 1)], res_ssem, res_rsem)
    sent_all(down_recv.at[pl.ds(0, pieces - 1)], down_ssem, down_rsem)


def finish(attention, layer, attention_out, layer_out):
    attention_out[...] = attention[...]
    layer_out[...] = layer[...]


def on_device(
    states,
    queries,
    new_keys,
    new_values,
    text_keys,
    text_values,
    text_length,
    image_keys,
    image_values,
    image_slot,
    block_list,
    block_count,
    image_first,
    image_count,
    out_weight,
    norm_gain,
    gate_weight,
    up_weight,
    down_weight,
):
    groups = lax.axis_size("group")
    depths = lax.axis_size("depth")
    mps = lax.axis_size("mp")
    pieces = groups * mps
    requests, heads, width = queries.shape
    listed = block_list.shape[1]
    copies = listed // (depths * groups)
    per_depth = requests // depths
    rows, model = states.shape
    cols = model // mps
    units = gate_weight.shape[1]
    span = text_keys.shape[2]
    part_cols = model // DOWN_CHUNKS
    dma = pltpu.SemaphoreType.DMA
    vmem = pl.BlockSpec(memory_space=pltpu.VMEM)
    hbm = pl.BlockSpec(memory_space=pl.ANY)
    small = (
        states,
        queries,
        new_keys,
        new_values,
        norm_gain.reshape(1, model),
        text_length,
        image_slot,
        block_list,
        block_count,
        image_first,
        image_count,
    )
    big = (
        text_keys,
        text_values,
        image_keys,
        image_values,
        out_weight,
        gate_weight,
        up_weight,
        down_weight,
    )
    scratch = [pltpu.VMEM(a.shape, a.dtype) for a in small[1:4]]
    scratch += [pltpu.VMEM((1, model), norm_gain.dtype)]
    scratch += [pltpu.SMEM(a.shape, a.dtype) for a in small[5:]]
    scratch += [pltpu.VMEM(a.shape, a.dtype) for a in big]
    scratch += [
        pltpu.SMEM((groups * copies,), I32),
        pltpu.SMEM((listed,), I32),
        pltpu.VMEM((mps, rows, cols), BF16),
        pltpu.VMEM((groups, copies, heads, width), BF16),
        pltpu.VMEM((groups, copies, heads, width), BF16),
        pltpu.VMEM((requests, heads, span), F32),
        pltpu.VMEM((requests, heads, width), F32),
        pltpu.VMEM((requests, heads, span), BF16),
        pltpu.VMEM((requests, 3, heads, width), F32),
        pltpu.VMEM((depths, per_depth, 3, heads, width), F32),
        pltpu.VMEM((groups, copies, heads, width), BF16),
        pltpu.VMEM((groups, 1, width), F32),
        pltpu.VMEM((depths * groups * copies, heads, width), BF16),
        pltpu.VMEM((depths * groups, 1, width), F32),
        pltpu.VMEM((per_depth, heads, width), F32),
        pltpu.VMEM((per_depth, heads * width), F32),
        pltpu.VMEM((mps, per_depth, cols), BF16),
        pltpu.VMEM((mps, per_depth, cols), BF16),
        pltpu.VMEM((per_depth, cols), F32),
        pltpu.VMEM((per_depth, cols), F32),
        pltpu.VMEM((mps, rows, cols), F32),
        pltpu.VMEM((mps, rows, cols), F32),
        pltpu.VMEM((pieces, per_depth, cols), BF16),
        pltpu.VMEM((groups * per_depth, width), F32),
        pltpu.VMEM((groups * per_depth, units), F32),
        pltpu.VMEM((groups * per_depth, units), F32),
        pltpu.VMEM((groups * per_depth, units), BF16),
        pltpu.VMEM((DOWN_CHUNKS, pieces, rows, part_cols), BF16),
        pltpu.VMEM((pieces, DOWN_CHUNKS, rows, part_cols), BF16),
        dma((len(big),)),
        dma((len(small),)),
        dma,
        dma,
        dma,
        dma((groups,)),
        dma,
        dma((depths,)),
        dma,
        dma,
        dma,
        dma,
        dma,
        dma,
        dma,
        dma((mps,)),
        dma,
        dma,
        dma,
        dma,
        dma,
        pltpu.SemaphoreType.REGULAR,
    ]
    raw = pl.pallas_call(
        functools.partial(kernel, (groups, depths, mps)),
        out_shape=(
            pltpu.VMEM((per_depth, heads, width), BF16),
            pltpu.VMEM((rows, model), BF16),
        ),
        in_specs=[hbm] * 19,
        out_specs=(vmem, vmem),
        scratch_shapes=scratch,
        compiler_params=pltpu.CompilerParams(
            collective_id=0, has_side_effects=True, vmem_limit_bytes=60000000
        ),
    )(*small, *big)
    return pl.pallas_call(
        finish,
        out_shape=(
            jax.ShapeDtypeStruct((per_depth, heads, width), BF16),
            jax.ShapeDtypeStruct((rows, model), BF16),
        ),
        in_specs=[vmem] * 2,
        out_specs=(vmem, vmem),
    )(*(pltpu.with_memory_space_constraint(r, pltpu.VMEM) for r in raw))


def solution(mesh):
    placed = (
        P(("group", "depth", "mp"), None),
        P("group", "mp", None),
        P("group", "mp", None),
        P("group", "mp", None),
        P("group", "mp", "depth", None),
        P("group", "mp", "depth", None),
        P("group"),
        P("group", "mp", None, None),
        P("group", "mp", None, None),
        P(),
        P(),
        P(),
        P("group"),
        P("group"),
        P("mp", None),
        P(),
        P(None, ("group", "mp")),
        P(None, ("group", "mp")),
        P(("group", "mp"), None),
    )
    return jax.shard_map(
        on_device,
        mesh=mesh,
        in_specs=placed,
        out_specs=(P(("group", "depth"), "mp", None), P(("group", "depth", "mp"), None)),
        check_vma=False,
    )
```
